32 devices in a mesh: grp: 4 (over z), seq: 4 (over y, x), mp: 2 (over core).
Axes of the slice: x: 2, y: 2, z: 4, core: 2. Of those that a mesh axis runs over, the one named last changes fastest.
Arguments:
- queries: bfloat16 [4, 1024, 2048], P('grp', 'seq', 'mp'), may hold values from -400 to 400
- neighbours: bfloat16 [4, 16, 256, 1024], P('grp', 'seq'), may hold values from -6 to 6
- w_key: bfloat16 [1024, 2048], P(('grp', 'seq'), 'mp'), may hold values from -0.1875 to 0.1875
- w_value: bfloat16 [1024, 2048], P(('grp', 'seq'), 'mp'), may hold values from -0.1875 to 0.1875
- lambdas: float32 [16], P('mp'), may hold values from 0.2 to 0.9
- gain: float32 [2048], P('mp'), may hold values from 0.5 to 1.5
- counts: int32 [4], P('grp'), may hold values from 2 to 16, as said below
- d_out: bfloat16 [4, 1024, 2048], P('grp', 'seq', 'mp'), may hold values from -6 to 6
Outputs:
- attended: bfloat16 [4, 1024, 2048], P('grp', 'seq', 'mp')
- d_neigh: float32 [4, 16, 256, 1024], P('grp', 'seq', None, 'mp')
The draws below stay inside these ranges and needn't reach their ends.
Inputs may be any that keep to these rules, and one draw needn't show every extreme that they name: `counts`: at least one sequence has all 16 groups valid.
All inputs are finite; a program needn't handle non-finite values.
Results may differ from the reference program's by a relative error of at most 0.017.
Values may be sent and summed in bfloat16 or wider, within the bound.
A program may use at most 128 MiB of HBM per device.

```python
import jax
import jax.numpy as jnp
from jax import lax

D_ENC = 1024
PAIRS = 16
KDIM = 64
VDIM = 128
GROUP = 64
NEIGH = 2
NLEN = 128
SEQS = 4
GROUPS = 16
TOKENS = 1024


def draw_queries(key, part):
    extent = (SEQS, TOKENS, PAIRS * 2 * KDIM)
    key_base = jax.random.fold_in(key, 11)
    sample = jax.random.truncated_normal(key_base, -6.0, 6.0, extent, jnp.float32)
    return sample.astype(jnp.bfloat16)


def draw_counts(key, part):
    key_base = jax.random.fold_in(key, 21)
    key_full = jax.random.fold_in(key, 22)
    ragged = jax.random.randint(key_base, (SEQS,), 2, GROUPS + 1, jnp.int32)
    full_seq = jax.random.randint(key_full, (), 0, SEQS, jnp.int32)
    which = jnp.arange(SEQS, dtype=jnp.int32)
    return jnp.where(which == full_seq, jnp.int32(GROUPS), ragged).astype(jnp.int32)


def steps_of(own_key, shape, cuts, least, high):
    factor_of, own = 1.0, jax.random.fold_in(own_key, 6)
    for dim, blocks in cuts:
        heights = jnp.exp(jax.random.uniform(jax.random.fold_in(own, dim), (blocks,), jnp.float32, least / len(cuts), high / len(cuts)))
        factor_of = factor_of * jnp.repeat(heights, shape[dim] // blocks).reshape([-1 if axis == dim else 1 for axis in range(len(shape))])
    return factor_of


def bell_draw(key, dims, spread, limit, shards=(), held_as=jnp.bfloat16):
    factor_of = steps_of(key, dims, shards, -0.22, 0.18) if shards else 1.0
    result = jax.random.normal(key, dims, jnp.float32) * spread * factor_of
    return jnp.minimum(jnp.maximum(result, -limit), limit).astype(held_as)


def setup_inputs(seed: int = 0) -> dict:
    keys = jax.random.split(jax.random.key(seed), 9)
    queries = draw_queries(jax.random.fold_in(keys[8], 71), 0)
    neighbours = bell_draw(keys[1], (SEQS, GROUPS, NEIGH * NLEN, D_ENC), 1.0, 6.0, ((0, 4), (1, 4)))
    w_key = bell_draw(keys[2], (D_ENC, PAIRS * 2 * KDIM), D_ENC ** -0.5, 0.1875, ((0, 16), (1, 2)))
    w_value = bell_draw(keys[3], (D_ENC, PAIRS * VDIM), D_ENC ** -0.5, 0.1875, ((0, 16), (1, 2)))
    lambdas = jnp.clip(0.2 + 0.7 * jax.random.uniform(keys[4], (PAIRS,), jnp.float32) ** steps_of(keys[4], (PAIRS,), ((0, 2),), -0.2, 0.2), 0.2, 0.9)
    gain = jnp.clip(1.0 + 0.1 * jax.random.normal(keys[5], (PAIRS * VDIM,), jnp.float32), 0.5, 1.5)
    counts = draw_counts(jax.random.fold_in(keys[8], 71), 0)
    d_out = bell_draw(keys[7], (SEQS, TOKENS, PAIRS * VDIM), 1.0, 6.0, ((0, 4), (1, 4), (2, 2)))
    return dict(queries=queries, neighbours=neighbours, w_key=w_key, w_value=w_value, lambdas=lambdas, gain=gain, counts=counts, d_out=d_out)


epsilon = 1e-06

def reference(queries, neighbours, w_key, w_value, lambdas, gain, counts, d_out):
    row_count = NEIGH * NLEN
    rows_all = GROUPS * row_count
    score_scale = KDIM ** (-0.5)
    gain_heads = gain.reshape(PAIRS, VDIM)
    lambda_b = lambdas[None, :, None, None]

    def one_sequence(items):
        encoded, query_rows, grad_rows, valid_count = items
        flat_enc = encoded.reshape(rows_all, D_ENC)
        key_own = jnp.dot(flat_enc, w_key, preferred_element_type=jnp.float32)
        value_own = jnp.dot(flat_enc, w_value, preferred_element_type=jnp.float32).astype(jnp.bfloat16)
        key_own = key_own.reshape(GROUPS, row_count, PAIRS, 2, KDIM)
        value_own = value_own.reshape(GROUPS, row_count, PAIRS, VDIM)
        key_heads = jnp.concatenate([jnp.zeros_like(key_own[:1]), key_own[:-1]], axis=0).astype(jnp.float32)
        value_heads = jnp.concatenate([jnp.zeros_like(value_own[:1]), value_own[:-1]], axis=0).astype(jnp.float32)
        query_heads = query_rows.reshape(GROUPS, GROUP, PAIRS, 2, KDIM).astype(jnp.float32)
        position = jnp.arange(GROUPS, dtype=jnp.int32)
        active = ((position >= 1) & (position < valid_count)).astype(jnp.float32)[:, None, None, None]
        scores = jnp.einsum('cqhmd,crhmd->chmqr', query_heads, key_heads, precision=lax.Precision.HIGHEST) * score_scale
        soft_maps = jax.nn.softmax(scores, axis=-1)
        mixed_w = (soft_maps[:, :, 0] - lambda_b * soft_maps[:, :, 1]).astype(jnp.bfloat16)
        heads = jnp.einsum('chqr,crhv->cqhv', mixed_w.astype(jnp.float32), value_heads)
        inverse = lax.rsqrt(lax.optimization_barrier(jnp.mean(heads * heads, axis=-1, keepdims=True)) + epsilon)
        normed = heads * inverse
        attended = (normed * gain_heads * active).astype(jnp.bfloat16).reshape(TOKENS, PAIRS * VDIM)
        upstream = grad_rows.reshape(GROUPS, GROUP, PAIRS, VDIM).astype(jnp.float32) * active
        d_normed = upstream * gain_heads
        d_heads = (inverse * (d_normed - normed * lax.optimization_barrier(jnp.mean(d_normed * normed, axis=-1, keepdims=True)))).astype(jnp.bfloat16)
        d_heads = d_heads.astype(jnp.float32)
        d_mixed = jnp.einsum('cqhv,crhv->chqr', d_heads, value_heads)
        d_values = jnp.einsum('chqr,cqhv->crhv', mixed_w.astype(jnp.float32), d_heads).astype(jnp.bfloat16)
        d_probs = jnp.stack([d_mixed, -lambda_b * d_mixed], axis=2)
        d_scores = (score_scale * soft_maps * (d_probs - lax.optimization_barrier(jnp.sum(d_probs * soft_maps, axis=-1, keepdims=True)))).astype(jnp.bfloat16)
        d_keys = jnp.einsum('chmqr,cqhmd->crhmd', d_scores.astype(jnp.float32), query_heads).astype(jnp.bfloat16)
        d_slots = jnp.dot(d_keys.reshape(rows_all, PAIRS * 2 * KDIM), w_key.T, preferred_element_type=jnp.float32)
        d_slots = d_slots + jnp.dot(d_values.reshape(rows_all, PAIRS * VDIM), w_value.T, preferred_element_type=jnp.float32)
        d_slots = d_slots.reshape(GROUPS, row_count, D_ENC)
        d_enc = jnp.concatenate([d_slots[1:], jnp.zeros_like(d_slots[:1])], axis=0)
        return (attended, d_enc)
    attended, d_neigh = lax.map(one_sequence, (neighbours, queries, d_out, counts))
    return (attended, d_neigh)
```

```python
import functools

import jax
import jax.numpy as jnp
from jax import lax
from jax.experimental import pallas as pl
from jax.experimental.pallas import tpu as pltpu
from jax.sharding import PartitionSpec as P

EPSILON = 1e-06
MESH = pl.DeviceIdType.MESH
NT = (((1,), (1,)), ((), ()))
TN = (((0,), (0,)), ((), ()))


def dot(left, right, dims=(((1,), (0,)), ((), ()))):
    return lax.dot_general(left, right, dims, preferred_element_type=jnp.float32)


def kernel(
    sizes,
    lambdas,
    counts,
    q_hbm,
    n_hbm,
    wk_hbm,
    wv_hbm,
    gain,
    do_hbm,
    att,
    d_out,
    x,
    qd,
    edge,
    w,
    acc,
    key,
    value,
    d_kv,
    att_out,
    att_in,
    send,
    got,
    local_sem,
    own_sem,
    z_send,
    z_recv,
    s_send,
    s_recv,
    r_send,
    r_recv,
    e_send,
    e_recv,
    a_send,
    a_recv,
    g_send,
    g_recv,
):
    n_grp, n_seq, n_mp, w_seq, chunks = sizes
    groups, rows, enc = x.shape
    group_len = qd.shape[1] // groups
    cols = w.shape[-1] // 2
    head_dim = cols // 2
    half = enc // n_mp
    grp_half = n_grp // n_mp
    grp, seq, mp = lax.axis_index("grp"), lax.axis_index("seq"), lax.axis_index("mp")
    w_pos = seq if w_seq > 1 else 0
    following = lax.rem(seq + 1, n_seq)
    preceding = lax.rem(seq + n_seq - 1, n_seq)
    ring = w_seq == 4
    if ring:
        right = lax.rem(seq, 2) * 2 + 1 - seq // 2
        left = (1 - lax.rem(seq, 2)) * 2 + seq // 2

    def at(c):
        return pl.ds(pl.multiple_of(c * cols, cols), cols)

    def own(c):
        return [
            pltpu.make_async_copy(
                src.at[:, at(c)], w.at[c, grp, w_pos, :, pl.ds(kind * cols, cols)], own_sem.at[c, kind]
            )
            for kind, src in enumerate((wk_hbm, wv_hbm))
        ]

    for c in range(chunks):
        for copy in own(c):
            copy.start()
    local = [
        pltpu.make_async_copy(q_hbm, qd.at[0], local_sem.at[0]),
        pltpu.make_async_copy(do_hbm, qd.at[1], local_sem.at[1]),
        pltpu.make_async_copy(n_hbm, x, local_sem.at[2]),
    ]
    for copy in local:
        copy.start()

    others = [{"grp": lax.rem(grp + o, n_grp)} for o in range(1, n_grp)]
    others += [{"seq": lax.rem(seq + o, n_seq)} for o in (range(1, n_seq) if w_seq > 1 else (1, n_seq - 1))]
    others += [{"mp": lax.rem(mp + o, n_mp)} for o in range(1, n_mp)]
    barrier = pltpu.get_barrier_semaphore()
    for device in others:
        pl.semaphore_signal(barrier, inc=1, device_id=device, device_id_type=MESH)
    pl.semaphore_wait(barrier, len(others))

    def remote(src, dst, send_sem, recv_sem, device):
        return pltpu.make_async_remote_copy(
            src_ref=src, dst_ref=dst, send_sem=send_sem, recv_sem=recv_sem, device_id=device, device_id_type=MESH
        )

    def over_grp(c):
        block = w.at[c, grp, w_pos]
        return [
            remote(block, block, z_send.at[c, o], z_recv.at[c, o], {"grp": lax.rem(grp + o, n_grp)})
            for o in range(1, n_grp)
        ]

    def over_seq(c):
        block = w.at[c, :, w_pos]
        if ring:
            targets = (right, left)
        else:
            targets = [lax.rem(seq + o, n_seq) for o in range(1, w_seq)]
        return [
            remote(block, block, s_send.at[c, i], s_recv.at[c, i], {"seq": target})
            for i, target in enumerate(targets)
        ]

    def relay(c):
        if not ring:
            return []
        copies = []
        for i, (source, target) in enumerate(((left, right), (right, left))):
            passed = w.at[c, :, source, :, pl.ds(i * cols, cols)]
            copies.append(remote(passed, passed, r_send.at[c, i], r_recv.at[c, i], {"seq": target}))
        return copies

    def edge_in(c):
        return remote(
            qd.at[:, pl.ds(0, group_len), at(c)],
            edge.at[:, :, at(c)],
            e_send.at[c],
            e_recv.at[c],
            {"seq": preceding},
        )

    def edge_out(c):
        return remote(
            att_out.at[:, at(c)], att_in.at[:, at(c)], a_send.at[c], a_recv.at[c], {"seq": following}
        )

    def start_grp(c):
        for copy in own(c):
            copy.wait()
        for copy in over_grp(c):
            copy.start()

    def start_seq(c):
        for copy in over_grp(c):
            copy.wait_recv()
        for copy in over_seq(c):
            copy.start()

    def start_relay(c):
        for arrival in over_seq(c):
            arrival.wait_recv()
        for copy in relay(c):
            copy.start()

    def start_edge(c):
        @pl.when(seq > 0)
        def _():
            edge_in(c).start()

    def arrived(c):
        for copy in relay(c):
            copy.wait_recv()

        @pl.when(seq < n_seq - 1)
        def _():
            edge_in(c).wait_recv()

    start_grp(0)
    start_grp(1)
    for copy in local[:2]:
        copy.wait()
    start_edge(0)
    start_edge(1)
    start_grp(2)

    @pl.when(seq == n_seq - 1)
    def _():
        edge[...] = jnp.zeros_like(edge)

    @pl.when(seq == 0)
    def _():
        att_in[...] = jnp.zeros_like(att_in)

    start_seq(0)
    acc[...] = jnp.zeros_like(acc)
    start_seq(1)
    start_relay(0)
    local[2].wait()

    scale = head_dim ** (-0.5)
    lane = lax.broadcasted_iota(jnp.int32, (group_len, cols), 1)
    on_first = lane < head_dim
    lane_row = lax.broadcasted_iota(jnp.int32, (1, 2 * group_len), 1)

    def project(c):
        weights = w[c].reshape(enc, 2 * cols)
        kv = dot(x[...].reshape(groups * rows, enc), weights)
        k = kv[:, :cols]
        hi = k.astype(jnp.bfloat16)
        key[:, :cols] = hi
        key[:, cols:] = (k - hi.astype(jnp.float32)).astype(jnp.bfloat16)
        value[...] = kv[:, cols:].astype(jnp.bfloat16)

    def attend(c, u):
        here = slice(u * rows, (u + 1) * rows)
        position = seq * groups + u + 1
        active = jnp.clip(counts[0] - position, 0, 1).astype(jnp.float32)
        lam = lambdas[c]
        if u < groups - 1:
            tokens = slice((u + 1) * group_len, (u + 2) * group_len)
            query = qd[0, tokens, at(c)]
            upstream = qd[1, tokens, at(c)]
        else:
            query = edge[0, :, at(c)]
            upstream = edge[1, :, at(c)]
        zero = jnp.zeros_like(query)
        q2 = jnp.concatenate([jnp.where(on_first, query, zero), jnp.where(on_first, zero, query)], axis=0)
        v = value[here, :]
        scores = dot(key[here, :], jnp.concatenate([q2, q2], axis=1), NT) * scale
        e = jnp.exp(scores - jnp.max(scores, axis=0, keepdims=True))
        weight = jnp.where(lane_row < group_len, jnp.float32(1.0), -lam)
        probs = e * (weight / jnp.sum(e, axis=0, keepdims=True))
        mix = (probs + pltpu.roll(probs, group_len, 1)).astype(jnp.bfloat16)
        heads = dot(mix, v, TN)[:group_len]
        inverse = lax.rsqrt(jnp.mean(heads * heads, axis=-1, keepdims=True) + EPSILON)
        normed = heads * inverse
        g = gain[:, at(c)]
        result = (normed * g * active).astype(jnp.bfloat16)
        if u < groups - 1:
            att[tokens, at(c)] = result
        else:
            att_out[:, at(c)] = result
        dn = upstream.astype(jnp.float32) * active * g
        d_heads = (inverse * (dn - normed * jnp.mean(dn * normed, axis=-1, keepdims=True))).astype(jnp.bfloat16)
        d_mix = dot(v, jnp.concatenate([d_heads, d_heads], axis=0), NT)
        total = jnp.sum(d_mix * probs, axis=0, keepdims=True) * (1.0 / weight)
        d_scores = (scale * probs * (d_mix - total)).astype(jnp.bfloat16)
        blank = jnp.zeros_like(q2)
        other = jnp.concatenate([d_heads, jnp.zeros_like(d_heads)], axis=0)
        right_side = jnp.concatenate(
            [jnp.concatenate([q2, blank], axis=1), jnp.concatenate([blank, other], axis=1)], axis=0
        )
        d_kv[here, :] = dot(jnp.concatenate([d_scores, mix], axis=1), right_side).astype(jnp.bfloat16)

    def weight_part(c, core):
        part = w[c, pl.ds(core * grp_half, grp_half)]
        return part.reshape(half, 2 * cols)

    def gradients(c):
        for core in range(n_mp):
            acc[core] += dot(d_kv[...], weight_part(c, core), NT)

    def step(c, first=False, final=False):
        if not final:

            @pl.when(c + 2 < chunks)
            def _():
                start_seq(c + 2)
                start_edge(c + 2)

            @pl.when(c + 3 < chunks)
            def _():
                start_grp(c + 3)

        arrived(c)
        project(c)
        if not final:
            start_relay(c + 1)
        if not first:
            gradients(c - 1)

            @pl.when(seq < n_seq - 1)
            def _():
                edge_out(c - 1).start()

        for u in range(groups):
            attend(c, u)

    step(0, first=True)

    def loop(c, carry):
        step(c)
        return carry

    lax.fori_loop(1, chunks - 1, loop, 0)
    last = chunks - 1
    step(last, final=True)

    pieces = send.shape[1]
    piece = send.shape[2]

    def exchange(o, i):
        return remote(
            send.at[o - 1, i], got.at[o - 1, i], g_send.at[o, i], g_recv.at[o, i], {"mp": lax.rem(mp + o, n_mp)}
        )

    for o in range(1, n_mp):
        core = lax.rem(mp + o, n_mp)
        for i in range(pieces):
            span = slice(i * piece, (i + 1) * piece)
            part = acc[core, span, :] + dot(d_kv[span, :], weight_part(last, core), NT)
            send[o - 1, i] = part.astype(jnp.bfloat16)
            exchange(o, i).start()

    @pl.when(seq < n_seq - 1)
    def _():
        edge_out(last).start()

    d_out[...] = acc[mp] + dot(d_kv[...], weight_part(last, mp), NT)

    @pl.when(seq > 0)
    def _():
        for c in range(chunks):
            edge_out(c).wait_recv()

    att[:group_len, :] = att_in[...]
    for i in range(pieces):
        span = slice(i * piece, (i + 1) * piece)
        total = d_out[span, :]
        for o in range(1, n_mp):
            exchange(o, i).wait()
            total += got[o - 1, i].astype(jnp.float32)
        d_out[span, :] = total

    def drain(c, carry):
        for copy in over_grp(c) + over_seq(c) + relay(c):
            copy.wait_send()

        @pl.when(seq > 0)
        def _():
            edge_in(c).wait_send()

        @pl.when(seq < n_seq - 1)
        def _():
            edge_out(c).wait_send()

        return carry

    lax.fori_loop(0, chunks, drain, 0)


def put_out(att, d_neigh, att_hbm, d_hbm, sem):
    copies = [
        pltpu.make_async_copy(d_neigh, d_hbm, sem.at[0]),
        pltpu.make_async_copy(att, att_hbm, sem.at[1]),
    ]
    for copy in copies:
        copy.start()
    for copy in copies:
        copy.wait()


def on_device(mesh_shape, queries, neighbours, w_key, w_value, lambdas, gain, counts, d_out):
    n_grp, n_seq, n_mp = (mesh_shape[name] for name in ("grp", "seq", "mp"))
    groups, rows, enc = neighbours.shape[1:]
    tokens, width = queries.shape[1:]
    w_seq = n_seq
    if w_key.shape[0] % 16:
        w_key = lax.all_gather(w_key, "seq", axis=0, tiled=True)
        w_value = lax.all_gather(w_value, "seq", axis=0, tiled=True)
        w_seq = 1
    w_rows = w_key.shape[0]
    chunks = lambdas.shape[0]
    cols = w_key.shape[1] // chunks
    half = enc // n_mp
    group_len = tokens // groups
    pieces = 2
    bf16, f32 = jnp.bfloat16, jnp.float32
    vmem = pl.BlockSpec(memory_space=pltpu.VMEM)
    smem = pl.BlockSpec(memory_space=pltpu.SMEM)
    hbm = pl.BlockSpec(memory_space=pl.ANY)
    dma = pltpu.SemaphoreType.DMA
    hops = max(2, w_seq)
    att, d_neigh = pl.pallas_call(
        functools.partial(kernel, (n_grp, n_seq, n_mp, w_seq, chunks)),
        out_shape=(
            pltpu.VMEM((tokens, width), bf16),
            pltpu.VMEM((groups * rows, half), f32),
        ),
        in_specs=[smem, smem, hbm, hbm, hbm, hbm, vmem, hbm],
        out_specs=(vmem, vmem),
        scratch_shapes=[
            pltpu.VMEM((groups, rows, enc), bf16),
            pltpu.VMEM((2, tokens, width), bf16),
            pltpu.VMEM((2, group_len, width), bf16),
            pltpu.VMEM((chunks, n_grp, w_seq, w_rows, 2 * cols), bf16),
            pltpu.VMEM((n_mp, groups * rows, half), f32),
            pltpu.VMEM((groups * rows, 2 * cols), bf16),
            pltpu.VMEM((groups * rows, cols), bf16),
            pltpu.VMEM((groups * rows, 2 * cols), bf16),
            pltpu.VMEM((group_len, width), bf16),
            pltpu.VMEM((group_len, width), bf16),
            pltpu.VMEM((n_mp - 1, pieces, groups * rows // pieces, half), bf16),
            pltpu.VMEM((n_mp - 1, pieces, groups * rows // pieces, half), bf16),
            dma((3,)),
            dma((chunks, 2)),
            dma((chunks, n_grp)),
            dma((chunks, n_grp)),
            dma((chunks, hops)),
            dma((chunks, hops)),
            dma((chunks, 2)),
            dma((chunks, 2)),
            dma((chunks,)),
            dma((chunks,)),
            dma((chunks,)),
            dma((chunks,)),
            dma((n_mp, pieces)),
            dma((n_mp, pieces)),
        ],
        compiler_params=pltpu.CompilerParams(
            collective_id=0, has_side_effects=True, vmem_limit_bytes=48 * 1024 * 1024
        ),
    )(lambdas, counts, queries[0], neighbours[0], w_key, w_value, gain.reshape(1, -1), d_out[0])
    att, d_neigh = pl.pallas_call(
        put_out,
        out_shape=(
            jax.ShapeDtypeStruct((tokens, width), bf16),
            jax.ShapeDtypeStruct((groups * rows, half), f32),
        ),
        in_specs=[vmem, vmem],
        out_specs=(hbm, hbm),
        scratch_shapes=[dma((2,))],
        compiler_params=pltpu.CompilerParams(vmem_limit_bytes=1024 * 1024),
    )(att, d_neigh)
    return att[None], d_neigh.reshape(1, groups, rows, half)


def solution(mesh):
    in_specs = (
        P("grp", "seq", "mp"),
        P("grp", "seq", None, None),
        P(("grp", "seq"), "mp"),
        P(("grp", "seq"), "mp"),
        P("mp"),
        P("mp"),
        P("grp"),
        P("grp", "seq", "mp"),
    )
    out_specs = (P("grp", "seq", "mp"), P("grp", "seq", None, "mp"))
    return jax.shard_map(
        functools.partial(on_device, dict(mesh.shape)),
        mesh=mesh,
        in_specs=in_specs,
        out_specs=out_specs,
        check_vma=False,
    )
```

```python
import functools

import jax
import jax.numpy as jnp
from jax import lax
from jax.experimental import pallas as pl
from jax.experimental.pallas import tpu as pltpu
from jax.sharding import PartitionSpec as P

EPSILON = 1e-06
TOGETHER = 4
MESH = pl.DeviceIdType.MESH
NT = (((1,), (1,)), ((), ()))
TN = (((0,), (0,)), ((), ()))


def dot(left, right, dims=(((1,), (0,)), ((), ()))):
    return lax.dot_general(left, right, dims, preferred_element_type=jnp.float32)


def kernel(
    sizes,
    lambdas,
    counts,
    q_hbm,
    n_hbm,
    wk_hbm,
    wv_hbm,
    gain,
    do_hbm,
    att,
    d_out,
    x,
    qd,
    edge,
    w,
    acc,
    key,
    value,
    d_kv,
    att_out,
    att_in,
    send,
    got,
    local_sem,
    own_sem,
    z_send,
    z_recv,
    s_send,
    s_recv,
    r_send,
    r_recv,
    e_send,
    e_recv,
    a_send,
    a_recv,
    g_send,
    g_recv,
):
    n_grp, n_seq, n_mp, w_seq, chunks = sizes
    groups, rows, enc = x.shape
    group_len = qd.shape[1] // groups
    cols = w.shape[-1] // 2
    head_dim = cols // 2
    half = enc // n_mp
    grp_half = n_grp // n_mp
    grp, seq, mp = lax.axis_index("grp"), lax.axis_index("seq"), lax.axis_index("mp")
    w_pos = seq if w_seq > 1 else 0
    following = lax.rem(seq + 1, n_seq)
    preceding = lax.rem(seq + n_seq - 1, n_seq)
    ring = w_seq == 4
    if ring:
        right = lax.rem(seq, 2) * 2 + 1 - seq // 2
        left = (1 - lax.rem(seq, 2)) * 2 + seq // 2

    def at(c):
        return pl.ds(pl.multiple_of(c * cols, cols), cols)

    def own(c):
        return [
            pltpu.make_async_copy(
                src.at[:, at(c)], w.at[c, grp, w_pos, :, pl.ds(kind * cols, cols)], own_sem.at[c, kind]
            )
            for kind, src in enumerate((wk_hbm, wv_hbm))
        ]

    for c in range(chunks):
        for copy in own(c):
            copy.start()
    local = [
        pltpu.make_async_copy(q_hbm, qd.at[0], local_sem.at[0]),
        pltpu.make_async_copy(do_hbm, qd.at[1], local_sem.at[1]),
        pltpu.make_async_copy(n_hbm, x, local_sem.at[2]),
    ]
    for copy in local:
        copy.start()

    others = [{"grp": lax.rem(grp + o, n_grp)} for o in range(1, n_grp)]
    others += [{"seq": lax.rem(seq + o, n_seq)} for o in (range(1, n_seq) if w_seq > 1 else (1, n_seq - 1))]
    others += [{"mp": lax.rem(mp + o, n_mp)} for o in range(1, n_mp)]
    barrier = pltpu.get_barrier_semaphore()
    for device in others:
        pl.semaphore_signal(barrier, inc=1, device_id=device, device_id_type=MESH)
    pl.semaphore_wait(barrier, len(others))

    def remote(src, dst, send_sem, recv_sem, device):
        return pltpu.make_async_remote_copy(
            src_ref=src, dst_ref=dst, send_sem=send_sem, recv_sem=recv_sem, device_id=device, device_id_type=MESH
        )

    if ring:
        targets = (right, left)
    else:
        targets = [lax.rem(seq + o, n_seq) for o in range(1, w_seq)]
    hops = range(1, n_grp)
    by_grp = chunks - 1 if ring and chunks > 4 else chunks

    def over_grp(c, whole=False):
        block = w.at[c, grp] if whole else w.at[c, grp, w_pos]
        return [
            remote(block, block, z_send.at[c, o], z_recv.at[c, o], {"grp": lax.rem(grp + o, n_grp)}) for o in hops
        ]

    def over_seq(c, o):
        block = w.at[c, lax.rem(grp + n_grp - o, n_grp), w_pos]
        return [
            remote(block, block, s_send.at[c, i, o], s_recv.at[c, i, o], {"seq": target})
            for i, target in enumerate(targets)
        ]

    def relay(c, grps=slice(None)):
        if not ring:
            return []
        copies = []
        for i, (source, target) in enumerate(((left, right), (right, left))):
            passed = w.at[c, grps, source, :, pl.ds(i * cols, cols)]
            copies.append(remote(passed, passed, r_send.at[c, i], r_recv.at[c, i], {"seq": target}))
        return copies

    def edge_in(c):
        return remote(
            qd.at[:, pl.ds(0, group_len), at(c)],
            edge.at[:, :, at(c)],
            e_send.at[c],
            e_recv.at[c],
            {"seq": preceding},
        )

    def edge_out(c):
        return remote(
            att_out.at[:, at(c)], att_in.at[:, at(c)], a_send.at[c], a_recv.at[c], {"seq": following}
        )

    def start(copies):
        for copy in copies:
            copy.start()

    def received(copies):
        for copy in copies:
            copy.wait_recv()

    def start_seq(c):
        for o, arrival in zip(hops, over_grp(c)):
            arrival.wait_recv()
            start(over_seq(c, o))

    def start_relay(c):
        for o in range(n_grp):
            received(over_seq(c, o))
        start(relay(c))

    def start_edge(c):
        @pl.when(seq > 0)
        def _():
            edge_in(c).start()

    def arrived(c, whole=False):
        if whole:
            received(over_grp(c, True))
        else:
            received(relay(c))

        @pl.when(seq < n_seq - 1)
        def _():
            edge_in(c).wait_recv()

    for c in [*range(by_grp, chunks), *range(by_grp)]:
        for copy in own(c):
            copy.wait()
        if c < by_grp:
            start(over_grp(c))
        start(over_seq(c, 0))
    for copy in local[:2]:
        copy.wait()
    for c in range(min(3, chunks)):
        start_edge(c)

    @pl.when(seq == n_seq - 1)
    def _():
        edge[...] = jnp.zeros_like(edge)

    @pl.when(seq == 0)
    def _():
        att_in[...] = jnp.zeros_like(att_in)

    acc[...] = jnp.zeros_like(acc)
    for c in range(by_grp, chunks):
        received(over_seq(c, 0))
        start(relay(c, grp))
    start_seq(0)
    for c in range(by_grp, chunks):
        received(relay(c, grp))
        start(over_grp(c, True))
    if by_grp > 1:
        start_seq(1)
    start_relay(0)
    if by_grp > 2:
        start_seq(2)
    local[2].wait()

    scale = head_dim ** (-0.5)
    lane = lax.broadcasted_iota(jnp.int32, (group_len, cols), 1)
    on_first = lane < head_dim
    lane_row = lax.broadcasted_iota(jnp.int32, (1, 2 * group_len), 1)

    def project(c):
        weights = w[c].reshape(enc, 2 * cols)
        states = x[...].reshape(groups * rows, enc)
        kv = dot(states[:, : enc // 2], weights[: enc // 2]) + dot(states[:, enc // 2 :], weights[enc // 2 :])
        k = kv[:, :cols]
        hi = k.astype(jnp.bfloat16)
        key[:, :cols] = hi
        key[:, cols:] = (k - hi.astype(jnp.float32)).astype(jnp.bfloat16)
        value[...] = kv[:, cols:].astype(jnp.bfloat16)

    def attend(c, slots):
        lam = lambdas[c]
        weight = jnp.where(lane_row < group_len, jnp.float32(1.0), -lam)
        unweight = 1.0 / weight
        g = gain[:, at(c)]
        blank = jnp.zeros((2 * group_len, cols), jnp.bfloat16)
        blank_half = jnp.zeros((group_len, cols), jnp.bfloat16)
        here = [slice(u * rows, (u + 1) * rows) for u in slots]
        tokens = [slice((u + 1) * group_len, (u + 2) * group_len) for u in slots]
        active = [jnp.clip(counts[0] - (seq * groups + u + 1), 0, 1).astype(jnp.float32) for u in slots]
        count = range(len(slots))

        def of_tokens(kind, i):
            if slots[i] < groups - 1:
                return qd[kind, tokens[i], at(c)]
            return edge[kind, :, at(c)]

        q2, scores = [], []
        for i in count:
            query = of_tokens(0, i)
            zero = jnp.zeros_like(query)
            q2.append(jnp.concatenate([jnp.where(on_first, query, zero), jnp.where(on_first, zero, query)], axis=0))
        for i in count:
            scores.append(dot(key[here[i], :], jnp.concatenate([q2[i], q2[i]], axis=1), NT) * scale)
        e = [jnp.exp(scores[i] - jnp.max(scores[i], axis=0, keepdims=True)) for i in count]
        probs = [e[i] * (weight / jnp.sum(e[i], axis=0, keepdims=True)) for i in count]
        mix = [(probs[i] + pltpu.roll(probs[i], group_len, 1)).astype(jnp.bfloat16) for i in count]
        heads = [dot(mix[i], value[here[i], :], TN)[:group_len] for i in count]
        inverse = [lax.rsqrt(jnp.mean(heads[i] * heads[i], axis=-1, keepdims=True) + EPSILON) for i in count]
        normed = [heads[i] * inverse[i] for i in count]
        dn = [of_tokens(1, i).astype(jnp.float32) * active[i] * g for i in count]
        d_heads = [
            (inverse[i] * (dn[i] - normed[i] * jnp.mean(dn[i] * normed[i], axis=-1, keepdims=True))).astype(
                jnp.bfloat16
            )
            for i in count
        ]
        d_mix = [dot(value[here[i], :], jnp.concatenate([d_heads[i], d_heads[i]], axis=0), NT) for i in count]
        for i in count:
            result = (normed[i] * g * active[i]).astype(jnp.bfloat16)
            if slots[i] < groups - 1:
                att[tokens[i], at(c)] = result
            else:
                att_out[:, at(c)] = result
        total = [jnp.sum(d_mix[i] * probs[i], axis=0, keepdims=True) * unweight for i in count]
        d_scores = [(scale * probs[i] * (d_mix[i] - total[i])).astype(jnp.bfloat16) for i in count]
        for i in count:
            other = jnp.concatenate([d_heads[i], blank_half], axis=0)
            right_side = jnp.concatenate(
                [jnp.concatenate([q2[i], blank], axis=1), jnp.concatenate([blank, other], axis=1)], axis=0
            )
            d_kv[here[i], :] = dot(jnp.concatenate([d_scores[i], mix[i]], axis=1), right_side).astype(jnp.bfloat16)

    def weight_part(c, core):
        part = w[c, pl.ds(core * grp_half, grp_half)]
        return part.reshape(half, 2 * cols)

    def gradients(c):
        for core in range(n_mp):
            acc[core] += dot(d_kv[...], weight_part(c, core), NT)

    def step(c, first=False, final=False):
        if not final:

            @pl.when(c + 1 < by_grp)
            def _():
                start_relay(c + 1)

            @pl.when(c + 3 < by_grp)
            def _():
                start_seq(c + 3)

            @pl.when(c + 3 < chunks)
            def _():
                start_edge(c + 3)

        if not first:

            @pl.when(seq < n_seq - 1)
            def _():
                edge_out(c - 1).start()

        arrived(c, final and by_grp < chunks)
        project(c)
        if not first:
            gradients(c - 1)
        for u in range(0, groups, TOGETHER):
            attend(c, list(range(u, min(u + TOGETHER, groups))))

    step(0, first=True)

    def loop(c, carry):
        step(c)
        return carry

    lax.fori_loop(1, chunks - 1, loop, 0)
    last = chunks - 1
    step(last, final=True)

    pieces = send.shape[1]
    piece = send.shape[2]

    def exchange(o, i):
        return remote(
            send.at[o - 1, i], got.at[o - 1, i], g_send.at[o, i], g_recv.at[o, i], {"mp": lax.rem(mp + o, n_mp)}
        )

    for o in range(1, n_mp):
        core = lax.rem(mp + o, n_mp)
        for i in range(pieces):
            span = slice(i * piece, (i + 1) * piece)
            part = acc[core, span, :] + dot(d_kv[span, :], weight_part(last, core), NT)
            send[o - 1, i] = part.astype(jnp.bfloat16)
            exchange(o, i).start()

    @pl.when(seq < n_seq - 1)
    def _():
        edge_out(last).start()

    d_out[...] = acc[mp] + dot(d_kv[...], weight_part(last, mp), NT)

    @pl.when(seq > 0)
    def _():
        for c in range(chunks):
            edge_out(c).wait_recv()

    att[:group_len, :] = att_in[...]
    for i in range(pieces):
        span = slice(i * piece, (i + 1) * piece)
        total = d_out[span, :]
        for o in range(1, n_mp):
            exchange(o, i).wait()
            total += got[o - 1, i].astype(jnp.float32)
        d_out[span, :] = total

    def sent(copies):
        for copy in copies:
            copy.wait_send()

    for c in range(by_grp, chunks):
        sent(over_grp(c, True))
        sent(over_seq(c, 0))
        sent(relay(c, grp))

    def drain_own(c, carry):
        sent(over_grp(c))
        for o in range(n_grp):
            sent(over_seq(c, o))
        sent(relay(c))
        return carry

    lax.fori_loop(0, by_grp, drain_own, 0)

    def drain(c, carry):
        @pl.when(seq > 0)
        def _():
            edge_in(c).wait_send()

        @pl.when(seq < n_seq - 1)
        def _():
            edge_out(c).wait_send()

        return carry

    lax.fori_loop(0, chunks, drain, 0)


def put_out(att, d_neigh, att_hbm, d_hbm, sem):
    copies = [
        pltpu.make_async_copy(d_neigh, d_hbm, sem.at[0]),
        pltpu.make_async_copy(att, att_hbm, sem.at[1]),
    ]
    for copy in copies:
        copy.start()
    for copy in copies:
        copy.wait()


def on_device(mesh_shape, queries, neighbours, w_key, w_value, lambdas, gain, counts, d_out):
    n_grp, n_seq, n_mp = (mesh_shape[name] for name in ("grp", "seq", "mp"))
    groups, rows, enc = neighbours.shape[1:]
    tokens, width = queries.shape[1:]
    w_seq = n_seq
    if w_key.shape[0] % 16:
        w_key = lax.all_gather(w_key, "seq", axis=0, tiled=True)
        w_value = lax.all_gather(w_value, "seq", axis=0, tiled=True)
        w_seq = 1
    w_rows = w_key.shape[0]
    chunks = lambdas.shape[0]
    cols = w_key.shape[1] // chunks
    half = enc // n_mp
    group_len = tokens // groups
    pieces = 2
    bf16, f32 = jnp.bfloat16, jnp.float32
    vmem = pl.BlockSpec(memory_space=pltpu.VMEM)
    smem = pl.BlockSpec(memory_space=pltpu.SMEM)
    hbm = pl.BlockSpec(memory_space=pltpu.HBM)
    dma = pltpu.SemaphoreType.DMA
    ways = max(2, w_seq)
    att, d_neigh = pl.pallas_call(
        functools.partial(kernel, (n_grp, n_seq, n_mp, w_seq, chunks)),
        out_shape=(
            pltpu.VMEM((tokens, width), bf16),
            pltpu.VMEM((groups * rows, half), f32),
        ),
        in_specs=[smem, smem, hbm, hbm, hbm, hbm, vmem, hbm],
        out_specs=(vmem, vmem),
        scratch_shapes=[
            pltpu.VMEM((groups, rows, enc), bf16),
            pltpu.VMEM((2, tokens, width), bf16),
            pltpu.VMEM((2, group_len, width), bf16),
            pltpu.VMEM((chunks, n_grp, w_seq, w_rows, 2 * cols), bf16),
            pltpu.VMEM((n_mp, groups * rows, half), f32),
            pltpu.VMEM((groups * rows, 2 * cols), bf16),
            pltpu.VMEM((groups * rows, cols), bf16),
            pltpu.VMEM((groups * rows, 2 * cols), bf16),
            pltpu.VMEM((group_len, width), bf16),
            pltpu.VMEM((group_len, width), bf16),
            pltpu.VMEM((n_mp - 1, pieces, groups * rows // pieces, half), bf16),
            pltpu.VMEM((n_mp - 1, pieces, groups * rows // pieces, half), bf16),
            dma((3,)),
            dma((chunks, 2)),
            dma((chunks, n_grp)),
            dma((chunks, n_grp)),
            dma((chunks, ways, n_grp)),
            dma((chunks, ways, n_grp)),
            dma((chunks, 2)),
            dma((chunks, 2)),
            dma((chunks,)),
            dma((chunks,)),
            dma((chunks,)),
            dma((chunks,)),
            dma((n_mp, pieces)),
            dma((n_mp, pieces)),
        ],
        compiler_params=pltpu.CompilerParams(
            collective_id=0, has_side_effects=True, vmem_limit_bytes=64400000
        ),
    )(lambdas, counts, queries[0], neighbours[0], w_key, w_value, gain.reshape(1, -1), d_out[0])
    att, d_neigh = pl.pallas_call(
        put_out,
        out_shape=(
            jax.ShapeDtypeStruct((tokens, width), bf16),
            jax.ShapeDtypeStruct((groups * rows, half), f32),
        ),
        in_specs=[vmem, vmem],
        out_specs=(hbm, hbm),
        scratch_shapes=[dma((2,))],
        compiler_params=pltpu.CompilerParams(vmem_limit_bytes=1024 * 1024),
    )(att, d_neigh)
    return att[None], d_neigh.reshape(1, groups, rows, half)


def solution(mesh):
    in_specs = (
        P("grp", "seq", "mp"),
        P("grp", "seq", None, None),
        P(("grp", "seq"), "mp"),
        P(("grp", "seq"), "mp"),
        P("mp"),
        P("mp"),
        P("grp"),
        P("grp", "seq", "mp"),
    )
    out_specs = (P("grp", "seq", "mp"), P("grp", "seq", None, "mp"))
    return jax.shard_map(
        functools.partial(on_device, dict(mesh.shape)),
        mesh=mesh,
        in_specs=in_specs,
        out_specs=out_specs,
        check_vma=False,
    )
```

```python
import functools

import jax
import jax.numpy as jnp
from jax import lax
from jax.experimental import pallas as pl
from jax.experimental.pallas import tpu as pltpu
from jax.sharding import PartitionSpec as P

EPSILON = 1e-06
TOGETHER = 4
MESH = pl.DeviceIdType.MESH
NT = (((1,), (1,)), ((), ()))
TN = (((0,), (0,)), ((), ()))


def dot(left, right, dims=(((1,), (0,)), ((), ()))):
    return lax.dot_general(left, right, dims, preferred_element_type=jnp.float32)


def kernel(
    sizes,
    lambdas_hbm,
    counts_hbm,
    q_hbm,
    n_hbm,
    wk_hbm,
    wv_hbm,
    gain_hbm,
    do_hbm,
    att,
    d_out,
    lambdas,
    counts,
    gain,
    x,
    qd,
    edge,
    w,
    acc,
    key,
    value,
    d_kv,
    att_out,
    att_in,
    send,
    got,
    local_sem,
    own_sem,
    z_send,
    z_recv,
    l_send,
    l_recv,
    s_send,
    s_recv,
    r_send,
    r_recv,
    e_send,
    e_recv,
    a_send,
    a_recv,
    g_send,
    g_recv,
):
    n_grp, n_seq, n_mp, w_seq, chunks = sizes
    groups, rows, enc = x.shape
    group_len = qd.shape[1] // groups
    cols = w.shape[-1] // 2
    head_dim = cols // 2
    half = enc // n_mp
    grp_half = n_grp // n_mp
    grp, seq, mp = lax.axis_index("grp"), lax.axis_index("seq"), lax.axis_index("mp")
    w_pos = seq if w_seq > 1 else 0
    following = lax.rem(seq + 1, n_seq)
    preceding = lax.rem(seq + n_seq - 1, n_seq)
    ring = w_seq == 4
    if ring:
        right = lax.rem(seq, 2) * 2 + 1 - seq // 2
        left = (1 - lax.rem(seq, 2)) * 2 + seq // 2

    def at(c):
        return pl.ds(pl.multiple_of(c * cols, cols), cols)

    def own(c):
        return [
            pltpu.make_async_copy(
                src.at[:, at(c)], w.at[c, grp, w_pos, :, pl.ds(kind * cols, cols)], own_sem.at[c, kind]
            )
            for kind, src in enumerate((wk_hbm, wv_hbm))
        ]

    for c in range(chunks):
        for copy in own(c):
            copy.start()
    local = [
        pltpu.make_async_copy(q_hbm, qd.at[0], local_sem.at[0]),
        pltpu.make_async_copy(do_hbm, qd.at[1], local_sem.at[1]),
        pltpu.make_async_copy(n_hbm, x, local_sem.at[2]),
        pltpu.make_async_copy(lambdas_hbm, lambdas, local_sem.at[3]),
        pltpu.make_async_copy(counts_hbm, counts, local_sem.at[4]),
        pltpu.make_async_copy(gain_hbm, gain, local_sem.at[5]),
    ]
    for copy in local:
        copy.start()

    others = [{"grp": lax.rem(grp + o, n_grp)} for o in range(1, n_grp)]
    others += [{"seq": lax.rem(seq + o, n_seq)} for o in (range(1, n_seq) if w_seq > 1 else (1, n_seq - 1))]
    others += [{"mp": lax.rem(mp + o, n_mp)} for o in range(1, n_mp)]
    barrier = pltpu.get_barrier_semaphore()
    for device in others:
        pl.semaphore_signal(barrier, inc=1, device_id=device, device_id_type=MESH)
    pl.semaphore_wait(barrier, len(others))

    def remote(src, dst, send_sem, recv_sem, device):
        return pltpu.make_async_remote_copy(
            src_ref=src, dst_ref=dst, send_sem=send_sem, recv_sem=recv_sem, device_id=device, device_id_type=MESH
        )

    if ring:
        targets = (right, left)
    else:
        targets = [lax.rem(seq + o, n_seq) for o in range(1, w_seq)]
    hops = range(1, n_grp)
    by_seq = 2 if ring and chunks >= 8 and n_grp <= 4 else 0
    by_grp = chunks - by_seq
    seq_first = range(by_grp - 1, chunks - 1) if by_seq else range(0)

    def nth(a):
        if not by_seq:
            return a
        if isinstance(a, int):
            return chunks - 1 if a == by_grp - 1 else a
        return jnp.where(a == by_grp - 1, chunks - 1, a)

    def over_grp(c):
        block = w.at[c, grp, w_pos]
        return [
            remote(block, block, z_send.at[c, o], z_recv.at[c, o], {"grp": lax.rem(grp + o, n_grp)}) for o in hops
        ]

    def line(c, k):
        ways = []
        for i, sign in enumerate((1, -1)):
            source, target = grp - sign * k, grp + sign
            block = w.at[c, jnp.clip(source, 0, n_grp - 1)]
            copy = remote(
                block,
                block,
                l_send.at[c, i, k],
                l_recv.at[c, i, k],
                {"grp": jnp.where(target < 0, 1, jnp.where(target >= n_grp, n_grp - 2, target))},
            )
            sends = (source >= 0) & (source < n_grp) & (target >= 0) & (target < n_grp)
            arrives = (source - sign >= 0) & (source - sign < n_grp)
            ways.append((copy, sends, arrives))
        return ways

    def start_line(c, k):
        if k:
            line_received(c, k - 1)
        for copy, sends, _ in line(c, k):
            pl.when(sends)(copy.start)

    def line_received(c, k):
        for copy, _, arrives in line(c, k):
            pl.when(arrives)(copy.wait_recv)

    def over_seq(c, o):
        block = w.at[c, lax.rem(grp + n_grp - o, n_grp), w_pos]
        return [
            remote(block, block, s_send.at[c, i, o], s_recv.at[c, i, o], {"seq": target})
            for i, target in enumerate(targets)
        ]

    def relay(c, grps=slice(None)):
        if not ring:
            return []
        copies = []
        for i, (source, target) in enumerate(((left, right), (right, left))):
            passed = w.at[c, grps, source, :, pl.ds(i * cols, cols)]
            copies.append(remote(passed, passed, r_send.at[c, i], r_recv.at[c, i], {"seq": target}))
        return copies

    def edge_in(c):
        return remote(
            qd.at[:, pl.ds(0, group_len), at(c)],
            edge.at[:, :, at(c)],
            e_send.at[c],
            e_recv.at[c],
            {"seq": preceding},
        )

    def edge_out(c):
        return remote(
            att_out.at[:, at(c)], att_in.at[:, at(c)], a_send.at[c], a_recv.at[c], {"seq": following}
        )

    def start(copies):
        for copy in copies:
            copy.start()

    def received(copies):
        for copy in copies:
            copy.wait_recv()

    def start_seq(c):
        for o, arrival in zip(hops, over_grp(c)):
            arrival.wait_recv()
            start(over_seq(c, o))

    def start_relay(c):
        for o in range(n_grp):
            received(over_seq(c, o))
        start(relay(c))

    def start_edge(c):
        @pl.when(seq > 0)
        def _():
            edge_in(c).start()

    def arrived(c, final):
        if not by_seq or final or isinstance(c, int):
            received(relay(c))
        else:

            @pl.when(c < by_grp - 1)
            def _():
                received(relay(c))

            @pl.when(c >= by_grp - 1)
            def _():
                line_received(c, n_grp - 2)

        @pl.when(seq < n_seq - 1)
        def _():
            edge_in(c).wait_recv()

    for c in seq_first:
        for copy in own(c):
            copy.wait()
        start(over_seq(c, 0))
    soon = min(4, by_grp)
    for a in range(by_grp):
        c = nth(a)
        for copy in own(c):
            copy.wait()
        if a < soon:
            start(over_grp(c))
        start(over_seq(c, 0))
    for copy in local[:2]:
        copy.wait()
    for c in range(min(3, chunks)):
        start_edge(c)

    @pl.when(seq == n_seq - 1)
    def _():
        edge[...] = jnp.zeros_like(edge)

    @pl.when(seq == 0)
    def _():
        att_in[...] = jnp.zeros_like(att_in)

    acc[...] = jnp.zeros_like(acc)
    for c in seq_first:
        received(over_seq(c, 0))
        start(relay(c, grp))
    start_seq(0)
    for c in seq_first:
        received(relay(c, grp))
        start_line(c, 0)
    for a in range(soon, by_grp):
        start(over_grp(nth(a)))
    if by_grp > 1:
        start_seq(1)
    start_relay(0)
    if by_grp > 2:
        start_seq(2)
    for copy in local[2:]:
        copy.wait()

    scale = head_dim ** (-0.5)
    lane = lax.broadcasted_iota(jnp.int32, (group_len, cols), 1)
    on_first = lane < head_dim
    lane_row = lax.broadcasted_iota(jnp.int32, (1, 2 * group_len), 1)

    def project(c):
        weights = w[c].reshape(enc, 2 * cols)
        states = x[...].reshape(groups * rows, enc)
        kv = dot(states[:, : enc // 2], weights[: enc // 2]) + dot(states[:, enc // 2 :], weights[enc // 2 :])
        k = kv[:, :cols]
        hi = k.astype(jnp.bfloat16)
        key[:, :cols] = hi
        key[:, cols:] = (k - hi.astype(jnp.float32)).astype(jnp.bfloat16)
        value[...] = kv[:, cols:].astype(jnp.bfloat16)

    def attend(c, slots):
        lam = lambdas[c]
        weight = jnp.where(lane_row < group_len, jnp.float32(1.0), -lam)
        unweight = 1.0 / weight
        g = gain[:, at(c)]
        blank = jnp.zeros((2 * group_len, cols), jnp.bfloat16)
        blank_half = jnp.zeros((group_len, cols), jnp.bfloat16)
        here = [slice(u * rows, (u + 1) * rows) for u in slots]
        tokens = [slice((u + 1) * group_len, (u + 2) * group_len) for u in slots]
        active = [jnp.clip(counts[0] - (seq * groups + u + 1), 0, 1).astype(jnp.float32) for u in slots]
        count = range(len(slots))

        def of_tokens(kind, i):
            if slots[i] < groups - 1:
                return qd[kind, tokens[i], at(c)]
            return edge[kind, :, at(c)]

        q2, scores = [], []
        for i in count:
            query = of_tokens(0, i)
            zero = jnp.zeros_like(query)
            q2.append(jnp.concatenate([jnp.where(on_first, query, zero), jnp.where(on_first, zero, query)], axis=0))
        for i in count:
            scores.append(dot(key[here[i], :], jnp.concatenate([q2[i], q2[i]], axis=1), NT) * scale)
        e = [jnp.exp(scores[i] - jnp.max(scores[i], axis=0, keepdims=True)) for i in count]
        probs = [e[i] * (weight / jnp.sum(e[i], axis=0, keepdims=True)) for i in count]
        mix = [(probs[i] + pltpu.roll(probs[i], group_len, 1)).astype(jnp.bfloat16) for i in count]
        heads = [dot(mix[i], value[here[i], :], TN)[:group_len] for i in count]
        inverse = [lax.rsqrt(jnp.mean(heads[i] * heads[i], axis=-1, keepdims=True) + EPSILON) for i in count]
        normed = [heads[i] * inverse[i] for i in count]
        dn = [of_tokens(1, i).astype(jnp.float32) * active[i] * g for i in count]
        d_heads = [
            (inverse[i] * (dn[i] - normed[i] * jnp.mean(dn[i] * normed[i], axis=-1, keepdims=True))).astype(
                jnp.bfloat16
            )
            for i in count
        ]
        d_mix = [dot(value[here[i], :], jnp.concatenate([d_heads[i], d_heads[i]], axis=0), NT) for i in count]
        for i in count:
            result = (normed[i] * g * active[i]).astype(jnp.bfloat16)
            if slots[i] < groups - 1:
                att[tokens[i], at(c)] = result
            else:
                att_out[:, at(c)] = result
        total = [jnp.sum(d_mix[i] * probs[i], axis=0, keepdims=True) * unweight for i in count]
        d_scores = [(scale * probs[i] * (d_mix[i] - total[i])).astype(jnp.bfloat16) for i in count]
        for i in count:
            other = jnp.concatenate([d_heads[i], blank_half], axis=0)
            right_side = jnp.concatenate(
                [jnp.concatenate([q2[i], blank], axis=1), jnp.concatenate([blank, other], axis=1)], axis=0
            )
            d_kv[here[i], :] = dot(jnp.concatenate([d_scores[i], mix[i]], axis=1), right_side).astype(jnp.bfloat16)

    def weight_part(c, core):
        part = w[c, pl.ds(core * grp_half, grp_half)]
        return part.reshape(half, 2 * cols)

    def gradients(c):
        for core in range(n_mp):
            acc[core] += dot(d_kv[...], weight_part(c, core), NT)

    def step(c, first=False, final=False):
        if not final:

            @pl.when(c + 1 < by_grp)
            def _():
                start_relay(nth(c + 1))

            @pl.when(c + 3 < by_grp)
            def _():
                start_seq(nth(c + 3))

            if by_seq and not first:
                for k in range(1, n_grp - 1):

                    @pl.when(c == 2 * k - 1)
                    def _(k=k):
                        for b in seq_first:
                            start_line(b, k)

            @pl.when(c + 3 < chunks)
            def _():
                start_edge(c + 3)

        if not first:

            @pl.when(seq < n_seq - 1)
            def _():
                edge_out(c - 1).start()

        arrived(c, final)
        project(c)
        if not first:
            gradients(c - 1)
        for u in range(0, groups, TOGETHER):
            attend(c, list(range(u, min(u + TOGETHER, groups))))

    step(0, first=True)

    def loop(c, carry):
        step(c)
        return carry

    lax.fori_loop(1, chunks - 1, loop, 0)
    last = chunks - 1
    step(last, final=True)

    pieces = send.shape[1]
    piece = send.shape[2]

    def exchange(o, i):
        return remote(
            send.at[o - 1, i], got.at[o - 1, i], g_send.at[o, i], g_recv.at[o, i], {"mp": lax.rem(mp + o, n_mp)}
        )

    for o in range(1, n_mp):
        core = lax.rem(mp + o, n_mp)
        for i in range(pieces):
            span = slice(i * piece, (i + 1) * piece)
            part = acc[core, span, :] + dot(d_kv[span, :], weight_part(last, core), NT)
            send[o - 1, i] = part.astype(jnp.bfloat16)
            exchange(o, i).start()

    @pl.when(seq < n_seq - 1)
    def _():
        edge_out(last).start()

    d_out[...] = acc[mp] + dot(d_kv[...], weight_part(last, mp), NT)

    @pl.when(seq > 0)
    def _():
        for c in range(chunks):
            edge_out(c).wait_recv()

    att[:group_len, :] = att_in[...]
    for i in range(pieces):
        span = slice(i * piece, (i + 1) * piece)
        total = d_out[span, :]
        for o in range(1, n_mp):
            exchange(o, i).wait()
            total += got[o - 1, i].astype(jnp.float32)
        d_out[span, :] = total

    def sent(copies):
        for copy in copies:
            copy.wait_send()

    for c in seq_first:
        sent(over_seq(c, 0))
        sent(relay(c, grp))
        for k in range(n_grp - 1):
            for copy, sends, _ in line(c, k):
                pl.when(sends)(copy.wait_send)

    def drain_own(a, carry):
        c = nth(a)
        sent(over_grp(c))
        for o in range(n_grp):
            sent(over_seq(c, o))
        sent(relay(c))
        return carry

    lax.fori_loop(0, by_grp, drain_own, 0)

    def drain(c, carry):
        @pl.when(seq > 0)
        def _():
            edge_in(c).wait_send()

        @pl.when(seq < n_seq - 1)
        def _():
            edge_out(c).wait_send()

        return carry

    lax.fori_loop(0, chunks, drain, 0)


def put_out(att, d_neigh, att_hbm, d_hbm, sem):
    copies = [
        pltpu.make_async_copy(d_neigh, d_hbm, sem.at[0]),
        pltpu.make_async_copy(att, att_hbm, sem.at[1]),
    ]
    for copy in copies:
        copy.start()
    for copy in copies:
        copy.wait()


def on_device(mesh_shape, queries, neighbours, w_key, w_value, lambdas, gain, counts, d_out):
    n_grp, n_seq, n_mp = (mesh_shape[name] for name in ("grp", "seq", "mp"))
    groups, rows, enc = neighbours.shape[1:]
    tokens, width = queries.shape[1:]
    w_seq = n_seq
    if w_key.shape[0] % 16:
        w_key = lax.all_gather(w_key, "seq", axis=0, tiled=True)
        w_value = lax.all_gather(w_value, "seq", axis=0, tiled=True)
        w_seq = 1
    w_rows = w_key.shape[0]
    chunks = lambdas.shape[0]
    cols = w_key.shape[1] // chunks
    half = enc // n_mp
    group_len = tokens // groups
    pieces = 2
    bf16, f32 = jnp.bfloat16, jnp.float32
    vmem = pl.BlockSpec(memory_space=pltpu.VMEM)
    hbm = pl.BlockSpec(memory_space=pltpu.HBM)
    dma = pltpu.SemaphoreType.DMA
    ways = max(2, w_seq)
    att, d_neigh = pl.pallas_call(
        functools.partial(kernel, (n_grp, n_seq, n_mp, w_seq, chunks)),
        out_shape=(
            pltpu.VMEM((tokens, width), bf16),
            pltpu.VMEM((groups * rows, half), f32),
        ),
        in_specs=[hbm] * 8,
        out_specs=(vmem, vmem),
        scratch_shapes=[
            pltpu.SMEM((chunks,), f32),
            pltpu.SMEM((1,), jnp.int32),
            pltpu.VMEM((1, width), f32),
            pltpu.VMEM((groups, rows, enc), bf16),
            pltpu.VMEM((2, tokens, width), bf16),
            pltpu.VMEM((2, group_len, width), bf16),
            pltpu.VMEM((chunks, n_grp, w_seq, w_rows, 2 * cols), bf16),
            pltpu.VMEM((n_mp, groups * rows, half), f32),
            pltpu.VMEM((groups * rows, 2 * cols), bf16),
            pltpu.VMEM((groups * rows, cols), bf16),
            pltpu.VMEM((groups * rows, 2 * cols), bf16),
            pltpu.VMEM((group_len, width), bf16),
            pltpu.VMEM((group_len, width), bf16),
            pltpu.VMEM((n_mp - 1, pieces, groups * rows // pieces, half), bf16),
            pltpu.VMEM((n_mp - 1, pieces, groups * rows // pieces, half), bf16),
            dma((6,)),
            dma((chunks, 2)),
            dma((chunks, n_grp)),
            dma((chunks, n_grp)),
            dma((chunks, 2, n_grp)),
            dma((chunks, 2, n_grp)),
            dma((chunks, ways, n_grp)),
            dma((chunks, ways, n_grp)),
            dma((chunks, 2)),
            dma((chunks, 2)),
            dma((chunks,)),
            dma((chunks,)),
            dma((chunks,)),
            dma((chunks,)),
            dma((n_mp, pieces)),
            dma((n_mp, pieces)),
        ],
        compiler_params=pltpu.CompilerParams(
            collective_id=0, has_side_effects=True, vmem_limit_bytes=64400000
        ),
    )(lambdas, counts, queries[0], neighbours[0], w_key, w_value, gain.reshape(1, -1), d_out[0])
    att, d_neigh = pl.pallas_call(
        put_out,
        out_shape=(
            jax.ShapeDtypeStruct((tokens, width), bf16),
            jax.ShapeDtypeStruct((groups * rows, half), f32),
        ),
        in_specs=[vmem, vmem],
        out_specs=(hbm, hbm),
        scratch_shapes=[dma((2,))],
        compiler_params=pltpu.CompilerParams(vmem_limit_bytes=1024 * 1024),
    )(att, d_neigh)
    return att[None], d_neigh.reshape(1, groups, rows, half)


def solution(mesh):
    in_specs = (
        P("grp", "seq", "mp"),
        P("grp", "seq", None, None),
        P(("grp", "seq"), "mp"),
        P(("grp", "seq"), "mp"),
        P("mp"),
        P("mp"),
        P("grp"),
        P("grp", "seq", "mp"),
    )
    out_specs = (P("grp", "seq", "mp"), P("grp", "seq", None, "mp"))
    return jax.shard_map(
        functools.partial(on_device, dict(mesh.shape)),
        mesh=mesh,
        in_specs=in_specs,
        out_specs=out_specs,
        check_vma=False,
    )
```

```python
import functools

import jax
import jax.numpy as jnp
from jax import lax
from jax.experimental import pallas as pl
from jax.experimental.pallas import tpu as pltpu
from jax.sharding import PartitionSpec as P

EPSILON = 1e-06
TOGETHER = 4
MESH = pl.DeviceIdType.MESH
NT = (((1,), (1,)), ((), ()))
TN = (((0,), (0,)), ((), ()))


def dot(left, right, dims=(((1,), (0,)), ((), ()))):
    return lax.dot_general(left, right, dims, preferred_element_type=jnp.float32)


def kernel(
    sizes,
    lambdas_hbm,
    counts_hbm,
    q_hbm,
    n_hbm,
    wk_hbm,
    wv_hbm,
    gain_hbm,
    do_hbm,
    att,
    d_out,
    lambdas,
    counts,
    gain,
    x,
    qd,
    edge,
    w,
    acc,
    key,
    value,
    d_kv,
    att_out,
    att_in,
    send,
    got,
    local_sem,
    own_sem,
    z_send,
    z_recv,
    l_send,
    l_recv,
    s_send,
    s_recv,
    r_send,
    r_recv,
    e_send,
    e_recv,
    a_send,
    a_recv,
    g_send,
    g_recv,
):
    n_grp, n_seq, n_mp, w_seq, chunks = sizes
    groups, rows, enc = x.shape
    group_len = qd.shape[1] // groups
    cols = w.shape[-1] // 2
    head_dim = cols // 2
    half = enc // n_mp
    grp_half = n_grp // n_mp
    grp, seq, mp = lax.axis_index("grp"), lax.axis_index("seq"), lax.axis_index("mp")
    w_pos = seq if w_seq > 1 else 0
    following = lax.rem(seq + 1, n_seq)
    preceding = lax.rem(seq + n_seq - 1, n_seq)
    ring = w_seq == 4
    if ring:
        right = lax.rem(seq, 2) * 2 + 1 - seq // 2
        left = (1 - lax.rem(seq, 2)) * 2 + seq // 2

    def at(c):
        return pl.ds(pl.multiple_of(c * cols, cols), cols)

    def own(c):
        return [
            pltpu.make_async_copy(
                src.at[:, at(c)], w.at[c, grp, w_pos, :, pl.ds(kind * cols, cols)], own_sem.at[c]
            )
            for kind, src in enumerate((wk_hbm, wv_hbm))
        ]

    def own_arrived(c):
        block = w.at[c, grp, w_pos]
        pltpu.make_async_copy(block, block, own_sem.at[c]).wait()

    for c in range(chunks):
        for copy in own(c):
            copy.start()
    local = [
        pltpu.make_async_copy(q_hbm, qd.at[0], local_sem.at[0]),
        pltpu.make_async_copy(do_hbm, qd.at[1], local_sem.at[1]),
        pltpu.make_async_copy(n_hbm, x, local_sem.at[2]),
        pltpu.make_async_copy(lambdas_hbm, lambdas, local_sem.at[3]),
        pltpu.make_async_copy(counts_hbm, counts, local_sem.at[4]),
        pltpu.make_async_copy(gain_hbm, gain, local_sem.at[5]),
    ]
    for copy in local:
        copy.start()

    others = [{"grp": lax.rem(grp + o, n_grp)} for o in range(1, n_grp)]
    others += [{"seq": lax.rem(seq + o, n_seq)} for o in (range(1, n_seq) if w_seq > 1 else (1, n_seq - 1))]
    others += [{"mp": lax.rem(mp + o, n_mp)} for o in range(1, n_mp)]
    barrier = pltpu.get_barrier_semaphore()
    for device in others:
        pl.semaphore_signal(barrier, inc=1, device_id=device, device_id_type=MESH)
    pl.semaphore_wait(barrier, len(others))

    def remote(src, dst, send_sem, recv_sem, device):
        return pltpu.make_async_remote_copy(
            src_ref=src, dst_ref=dst, send_sem=send_sem, recv_sem=recv_sem, device_id=device, device_id_type=MESH
        )

    if ring:
        targets = (right, left)
    else:
        targets = [lax.rem(seq + o, n_seq) for o in range(1, w_seq)]
    hops = range(1, n_grp)
    by_seq = 2 if ring and chunks >= 8 and n_grp <= 4 else 0
    by_grp = chunks - by_seq
    seq_first = (chunks - 4, chunks - 2) if by_seq else ()
    plain = by_grp - 2 if by_seq else by_grp

    def nth(a):
        late = 2 * a - plain + 1
        if isinstance(a, int):
            return a if a < plain else late
        return jnp.where(a < plain, a, late)

    def bulk(block, send_sem, recv_sem):
        return remote(block, block, send_sem, recv_sem, {"grp": lax.rem(grp + 1, n_grp)})

    def over_grp(c):
        block = w.at[c, grp, w_pos]
        return [
            remote(block, block, z_send.at[c], z_recv.at[c, o - 1], {"grp": lax.rem(grp + o, n_grp)}) for o in hops
        ]

    def line(c, k):
        ways = []
        b = (c - seq_first[0]) // (seq_first[1] - seq_first[0])
        for i, sign in enumerate((1, -1)):
            source, target = grp - sign * k, grp + sign
            block = w.at[c, jnp.clip(source, 0, n_grp - 1)]
            copy = remote(
                block,
                block,
                l_send.at[b, i, k],
                l_recv.at[b, i, k],
                {"grp": jnp.where(target < 0, 1, jnp.where(target >= n_grp, n_grp - 2, target))},
            )
            sends = (source >= 0) & (source < n_grp) & (target >= 0) & (target < n_grp)
            arrives = (source - sign >= 0) & (source - sign < n_grp)
            ways.append((copy, sends, arrives))
        return ways

    def start_line(c, k):
        if k:
            line_received(c, k - 1)
        for copy, sends, _ in line(c, k):
            pl.when(sends)(copy.start)

    def line_received(c, k):
        for copy, _, arrives in line(c, k):
            pl.when(arrives)(copy.wait_recv)

    def over_seq(c, o):
        block = w.at[c, lax.rem(grp + n_grp - o, n_grp), w_pos]
        return [
            remote(block, block, s_send.at[c], s_recv.at[c], {"seq": target}) for target in targets
        ]

    def all_seq(c, grps=slice(None)):
        return [bulk(w.at[c, grps, pl.ds(0, len(targets))], s_send.at[c], s_recv.at[c])] if targets else []

    def relay(c, grps=slice(None)):
        if not ring:
            return []
        copies = []
        for i, (source, target) in enumerate(((left, right), (right, left))):
            passed = w.at[c, grps, source, :, pl.ds(i * cols, cols)]
            copies.append(remote(passed, passed, r_send.at[c], r_recv.at[c], {"seq": target}))
        return copies

    def all_relay(c, grps=slice(None)):
        return [bulk(w.at[c, grps, 0], r_send.at[c], r_recv.at[c])] if ring else []

    def edge_in(c):
        return remote(
            qd.at[:, pl.ds(0, group_len), at(c)],
            edge.at[:, :, at(c)],
            e_send.at[0],
            e_recv.at[c],
            {"seq": preceding},
        )

    def edge_out(c):
        return remote(
            att_out.at[:, at(c)], att_in.at[:, at(c)], a_send.at[0], a_recv.at[0], {"seq": following}
        )

    def start(copies):
        for copy in copies:
            copy.start()

    def received(copies):
        for copy in copies:
            copy.wait_recv()

    def start_seq(c):
        for o, arrival in zip(hops, over_grp(c)):
            arrival.wait_recv()
            start(over_seq(c, o))

    def start_relay(c):
        received(all_seq(c))
        start(relay(c))

    def start_edge(c):
        @pl.when(seq > 0)
        def _():
            edge_in(c).start()

    def arrived(c):
        if isinstance(c, int):
            received(all_relay(c))
        elif not by_seq:
            received(all_relay(c))
        else:
            lined = (c == seq_first[0]) | (c == seq_first[1])

            @pl.when(jnp.logical_not(lined))
            def _():
                received(all_relay(c))

            @pl.when(lined)
            def _():
                line_received(c, n_grp - 2)

        @pl.when(seq < n_seq - 1)
        def _():
            edge_in(c).wait_recv()

    def own_seq(a):
        if a < by_grp:
            start(over_seq(nth(a), 0))

    def own_grp(a):
        own_arrived(nth(a))
        start(over_grp(nth(a)))

    for c in seq_first:
        own_arrived(c)
        start(over_seq(c, 0))
    own_grp(0)
    own_seq(0)
    for a in range(1, min(4, by_grp)):
        own_grp(a)
    own_seq(1)
    for copy in local[:2]:
        copy.wait()

    @pl.when(seq == n_seq - 1)
    def _():
        edge[...] = jnp.zeros_like(edge)

    @pl.when(seq == 0)
    def _():
        att_in[...] = jnp.zeros_like(att_in)

    acc[...] = jnp.zeros_like(acc)
    for c in seq_first:
        received(all_seq(c, 0))
        start(relay(c, grp))
    start_edge(0)
    if chunks > 1:
        start_edge(1)
    own_seq(2)
    start_seq(0)
    own_seq(3)
    for c in seq_first:
        received(all_relay(c, 0))
        start_line(c, 0)
    for a in range(4, by_grp):
        own_grp(a)
    if by_grp > 1:
        start_seq(1)
    start_relay(0)
    if chunks > 2:
        start_edge(2)
    own_seq(4)
    if by_grp > 2:
        start_seq(2)
    for a in range(5, by_grp):
        own_seq(a)
    for copy in local[2:]:
        copy.wait()

    scale = head_dim ** (-0.5)
    folded = scale.hex().startswith("0x1.0000000000000p")
    lane = lax.broadcasted_iota(jnp.int32, (group_len, cols), 1)
    on_first = lane < head_dim
    lane_row = lax.broadcasted_iota(jnp.int32, (1, 2 * group_len), 1)

    def project(c):
        weights = w[c].reshape(enc, 2 * cols)
        states = x[...].reshape(groups * rows, enc)
        kv = dot(states[:, : enc // 2], weights[: enc // 2]) + dot(states[:, enc // 2 :], weights[enc // 2 :])
        k = kv[:, :cols]
        hi = k.astype(jnp.bfloat16)
        key[:, :cols] = hi
        key[:, cols:] = (k - hi.astype(jnp.float32)).astype(jnp.bfloat16)
        value[...] = kv[:, cols:].astype(jnp.bfloat16)

    def attend(c, slots):
        lam = lambdas[c]
        weight = jnp.where(lane_row < group_len, jnp.float32(1.0), -lam)
        unweight = 1.0 / weight
        g = gain[:, at(c)]
        blank = jnp.zeros((2 * group_len, cols), jnp.bfloat16)
        blank_half = jnp.zeros((group_len, cols), jnp.bfloat16)
        here = [slice(u * rows, (u + 1) * rows) for u in slots]
        tokens = [slice((u + 1) * group_len, (u + 2) * group_len) for u in slots]
        active = [jnp.clip(counts[0] - (seq * groups + u + 1), 0, 1).astype(jnp.float32) for u in slots]
        count = range(len(slots))

        def of_tokens(kind, i):
            if slots[i] < groups - 1:
                return qd[kind, tokens[i], at(c)]
            return edge[kind, :, at(c)]

        q2, scores = [], []
        for i in count:
            query = of_tokens(0, i)
            if folded:
                query = (query.astype(jnp.float32) * scale).astype(jnp.bfloat16)
            zero = jnp.zeros_like(query)
            q2.append(jnp.concatenate([jnp.where(on_first, query, zero), jnp.where(on_first, zero, query)], axis=0))
        for i in count:
            scores.append(dot(key[here[i], :], jnp.concatenate([q2[i], q2[i]], axis=1), NT))
            if not folded:
                scores[i] = scores[i] * scale
        e = [jnp.exp(scores[i] - jnp.max(scores[i], axis=0, keepdims=True)) for i in count]
        probs = [e[i] * (weight / jnp.sum(e[i], axis=0, keepdims=True)) for i in count]
        mix = [(probs[i] + pltpu.roll(probs[i], group_len, 1)).astype(jnp.bfloat16) for i in count]
        heads = [dot(mix[i], value[here[i], :], TN)[:group_len] for i in count]
        inverse = [lax.rsqrt(jnp.mean(heads[i] * heads[i], axis=-1, keepdims=True) + EPSILON) for i in count]
        normed = [heads[i] * inverse[i] for i in count]
        dn = [of_tokens(1, i).astype(jnp.float32) * active[i] * g for i in count]
        d_heads = [
            (inverse[i] * (dn[i] - normed[i] * jnp.mean(dn[i] * normed[i], axis=-1, keepdims=True))).astype(
                jnp.bfloat16
            )
            for i in count
        ]
        d_mix = [dot(value[here[i], :], jnp.concatenate([d_heads[i], d_heads[i]], axis=0), NT) for i in count]
        for i in count:
            result = (normed[i] * g * active[i]).astype(jnp.bfloat16)
            if slots[i] < groups - 1:
                att[tokens[i], at(c)] = result
            else:
                att_out[:, at(c)] = result
        total = [jnp.sum(d_mix[i] * probs[i], axis=0, keepdims=True) * unweight for i in count]
        outer = probs if folded else [scale * probs[i] for i in count]
        d_scores = [(outer[i] * (d_mix[i] - total[i])).astype(jnp.bfloat16) for i in count]
        for i in count:
            d_kv[here[i], :cols] = dot(d_scores[i], q2[i]).astype(jnp.bfloat16)
            d_kv[here[i], cols:] = dot(mix[i], jnp.concatenate([d_heads[i], blank_half], axis=0)).astype(jnp.bfloat16)

    def weight_part(c, core):
        part = w[c, pl.ds(core * grp_half, grp_half)]
        return part.reshape(half, 2 * cols)

    def gradients(c):
        for core in range(n_mp):
            acc[core] += dot(d_kv[...], weight_part(c, core), NT)

    def lines(c, i):
        for k in range(1, n_grp - 1):

            @pl.when(c == 2 * k - 1)
            def _(k=k):
                start_line(seq_first[i], k)

    def step(c, first=False, final=False):
        if not final:

            @pl.when(c + 1 < min(plain + 1, by_grp))
            def _():
                start_relay(nth(c + 1))

            @pl.when(c + 3 < plain)
            def _():
                start_seq(nth(c + 3))

            if not first:

                @pl.when((c + 2 >= plain) & (c + 2 < by_grp))
                def _():
                    start_seq(nth(c + 2))

            @pl.when(c + 3 < chunks)
            def _():
                start_edge(c + 3)

        if not first:

            @pl.when(seq < n_seq - 1)
            def _():
                edge_out(c - 1).start()

        if by_seq and not first and not final:
            lines(c, 0)
        arrived(c)
        project(c)
        if not first:
            gradients(c - 1)
        if by_seq and not first and not final:
            lines(c, 1)

            @pl.when(c == plain)
            def _():
                start_relay(nth(plain + 1))

        for u in range(0, groups, TOGETHER):
            attend(c, list(range(u, min(u + TOGETHER, groups))))

    step(0, first=True)

    def loop(c, carry):
        step(c)
        return carry

    lax.fori_loop(1, chunks - 1, loop, 0)
    last = chunks - 1
    step(last, final=True)

    pieces = send.shape[1]
    piece = send.shape[2]

    def exchange(o, i):
        return remote(
            send.at[o - 1, i], got.at[o - 1, i], g_send.at[o - 1, i], g_recv.at[o - 1, i], {"mp": lax.rem(mp + o, n_mp)}
        )

    for o in range(1, n_mp):
        core = lax.rem(mp + o, n_mp)
        for i in range(pieces):
            span = slice(i * piece, (i + 1) * piece)
            part = acc[core, span, :] + dot(d_kv[span, :], weight_part(last, core), NT)
            send[o - 1, i] = part.astype(jnp.bfloat16)
            exchange(o, i).start()

    @pl.when(seq < n_seq - 1)
    def _():
        edge_out(last).start()

    d_out[...] = acc[mp] + dot(d_kv[...], weight_part(last, mp), NT)

    @pl.when(seq > 0)
    def _():
        bulk(att_in, a_send.at[0], a_recv.at[0]).wait_recv()

    att[:group_len, :] = att_in[...]
    for i in range(pieces):
        span = slice(i * piece, (i + 1) * piece)
        total = d_out[span, :]
        for o in range(1, n_mp):
            exchange(o, i).wait()
            total += got[o - 1, i].astype(jnp.float32)
        d_out[span, :] = total

    def sent(copies):
        for copy in copies:
            copy.wait_send()

    for c in seq_first:
        sent(all_seq(c, 0))
        sent(all_relay(c, 0))
        for k in range(n_grp - 1):
            for copy, sends, _ in line(c, k):
                pl.when(sends)(copy.wait_send)

    for a in range(by_grp):
        c = nth(a)
        bulk(w.at[c, pl.ds(0, n_grp - 1), w_pos], z_send.at[c], z_recv.at[c, 0]).wait_send()
        sent(all_seq(c))
        sent(all_relay(c))

    @pl.when(seq > 0)
    def _():
        bulk(edge, e_send.at[0], e_recv.at[0]).wait_send()

    @pl.when(seq < n_seq - 1)
    def _():
        bulk(att_in, a_send.at[0], a_recv.at[0]).wait_send()


def put_out(att, d_neigh, att_hbm, d_hbm, sem):
    copies = [
        pltpu.make_async_copy(d_neigh, d_hbm, sem.at[0]),
        pltpu.make_async_copy(att, att_hbm, sem.at[1]),
    ]
    for copy in copies:
        copy.start()
    for copy in copies:
        copy.wait()


def on_device(mesh_shape, queries, neighbours, w_key, w_value, lambdas, gain, counts, d_out):
    n_grp, n_seq, n_mp = (mesh_shape[name] for name in ("grp", "seq", "mp"))
    groups, rows, enc = neighbours.shape[1:]
    tokens, width = queries.shape[1:]
    w_seq = n_seq
    if w_key.shape[0] % 16:
        w_key = lax.all_gather(w_key, "seq", axis=0, tiled=True)
        w_value = lax.all_gather(w_value, "seq", axis=0, tiled=True)
        w_seq = 1
    w_rows = w_key.shape[0]
    chunks = lambdas.shape[0]
    cols = w_key.shape[1] // chunks
    half = enc // n_mp
    group_len = tokens // groups
    pieces = 2
    bf16, f32 = jnp.bfloat16, jnp.float32
    vmem = pl.BlockSpec(memory_space=pltpu.VMEM)
    hbm = pl.BlockSpec(memory_space=pltpu.HBM)
    dma = pltpu.SemaphoreType.DMA
    att, d_neigh = pl.pallas_call(
        functools.partial(kernel, (n_grp, n_seq, n_mp, w_seq, chunks)),
        out_shape=(
            pltpu.VMEM((tokens, width), bf16),
            pltpu.VMEM((groups * rows, half), f32),
        ),
        in_specs=[hbm] * 8,
        out_specs=(vmem, vmem),
        scratch_shapes=[
            pltpu.SMEM((chunks,), f32),
            pltpu.SMEM((1,), jnp.int32),
            pltpu.VMEM((1, width), f32),
            pltpu.VMEM((groups, rows, enc), bf16),
            pltpu.VMEM((2, tokens, width), bf16),
            pltpu.VMEM((2, group_len, width), bf16),
            pltpu.VMEM((chunks, n_grp, w_seq, w_rows, 2 * cols), bf16),
            pltpu.VMEM((n_mp, groups * rows, half), f32),
            pltpu.VMEM((groups * rows, 2 * cols), bf16),
            pltpu.VMEM((groups * rows, cols), bf16),
            pltpu.VMEM((groups * rows, 2 * cols), bf16),
            pltpu.VMEM((group_len, width), bf16),
            pltpu.VMEM((group_len, width), bf16),
            pltpu.VMEM((n_mp - 1, pieces, groups * rows // pieces, half), bf16),
            pltpu.VMEM((n_mp - 1, pieces, groups * rows // pieces, half), bf16),
            dma((6,)),
            dma((chunks,)),
            dma((chunks,)),
            dma((chunks, n_grp - 1)),
            dma((2, 2, n_grp - 1)),
            dma((2, 2, n_grp - 1)),
            dma((chunks,)),
            dma((chunks,)),
            dma((chunks,)),
            dma((chunks,)),
            dma((1,)),
            dma((chunks,)),
            dma((1,)),
            dma((1,)),
            dma((n_mp - 1, pieces)),
            dma((n_mp - 1, pieces)),
        ],
        compiler_params=pltpu.CompilerParams(
            collective_id=0, has_side_effects=True, vmem_limit_bytes=64400000
        ),
    )(lambdas, counts, queries[0], neighbours[0], w_key, w_value, gain.reshape(1, -1), d_out[0])
    att, d_neigh = pl.pallas_call(
        put_out,
        out_shape=(
            jax.ShapeDtypeStruct((tokens, width), bf16),
            jax.ShapeDtypeStruct((groups * rows, half), f32),
        ),
        in_specs=[vmem, vmem],
        out_specs=(hbm, hbm),
        scratch_shapes=[dma((2,))],
        compiler_params=pltpu.CompilerParams(vmem_limit_bytes=1024 * 1024),
    )(att, d_neigh)
    return att[None], d_neigh.reshape(1, groups, rows, half)


def solution(mesh):
    in_specs = (
        P("grp", "seq", "mp"),
        P("grp", "seq", None, None),
        P(("grp", "seq"), "mp"),
        P(("grp", "seq"), "mp"),
        P("mp"),
        P("mp"),
        P("grp"),
        P("grp", "seq", "mp"),
    )
    out_specs = (P("grp", "seq", "mp"), P("grp", "seq", None, "mp"))
    return jax.shard_map(
        functools.partial(on_device, dict(mesh.shape)),
        mesh=mesh,
        in_specs=in_specs,
        out_specs=out_specs,
        check_vma=False,
    )
```

```python
import functools

import jax
import jax.numpy as jnp
from jax import lax
from jax.experimental import pallas as pl
from jax.experimental.pallas import tpu as pltpu
from jax.sharding import PartitionSpec as P

EPSILON = 1e-06
TOGETHER = 4
MESH = pl.DeviceIdType.MESH
NT = (((1,), (1,)), ((), ()))
TN = (((0,), (0,)), ((), ()))


def dot(left, right, dims=(((1,), (0,)), ((), ()))):
    return lax.dot_general(left, right, dims, preferred_element_type=jnp.float32)


def kernel(
    sizes,
    lambdas_hbm,
    counts_hbm,
    q_hbm,
    n_hbm,
    wk_hbm,
    wv_hbm,
    gain_hbm,
    do_hbm,
    att,
    d_out,
    lambdas,
    counts,
    gain,
    x,
    qd,
    edge,
    w,
    acc,
    key,
    value,
    d_kv,
    att_out,
    att_in,
    send,
    got,
    local_sem,
    own_sem,
    z_send,
    z_recv,
    l_send,
    l_recv,
    s_send,
    s_recv,
    r_send,
    r_recv,
    e_send,
    e_recv,
    a_send,
    a_recv,
    g_send,
    g_recv,
):
    n_grp, n_seq, n_mp, w_seq, chunks = sizes
    groups, rows, enc = x.shape
    group_len = qd.shape[1] // groups
    cols = w.shape[-1] // 2
    head_dim = cols // 2
    half = enc // n_mp
    grp_half = n_grp // n_mp
    grp, seq, mp = lax.axis_index("grp"), lax.axis_index("seq"), lax.axis_index("mp")
    w_pos = seq if w_seq > 1 else 0
    following = lax.rem(seq + 1, n_seq)
    preceding = lax.rem(seq + n_seq - 1, n_seq)
    ring = w_seq == 4
    if ring:
        right = lax.rem(seq, 2) * 2 + 1 - seq // 2
        left = (1 - lax.rem(seq, 2)) * 2 + seq // 2

    def at(c):
        return pl.ds(pl.multiple_of(c * cols, cols), cols)

    def own(c):
        return [
            pltpu.make_async_copy(
                src.at[:, at(c)], w.at[c, grp, w_pos, :, pl.ds(kind * cols, cols)], own_sem.at[0]
            )
            for kind, src in enumerate((wk_hbm, wv_hbm))
        ]

    def own_arrived():
        block = w.at[:, grp, w_pos]
        pltpu.make_async_copy(block, block, own_sem.at[0]).wait()

    for c in range(chunks):
        for copy in own(c):
            copy.start()
    local = [
        pltpu.make_async_copy(q_hbm, qd.at[0], local_sem.at[0]),
        pltpu.make_async_copy(do_hbm, qd.at[1], local_sem.at[1]),
        pltpu.make_async_copy(n_hbm, x, local_sem.at[2]),
        pltpu.make_async_copy(lambdas_hbm, lambdas, local_sem.at[3]),
        pltpu.make_async_copy(counts_hbm, counts, local_sem.at[4]),
        pltpu.make_async_copy(gain_hbm, gain, local_sem.at[5]),
    ]
    for copy in local:
        copy.start()

    others = [{"grp": lax.rem(grp + o, n_grp)} for o in range(1, n_grp)]
    others += [{"seq": lax.rem(seq + o, n_seq)} for o in (range(1, n_seq) if w_seq > 1 else (1, n_seq - 1))]
    others += [{"mp": lax.rem(mp + o, n_mp)} for o in range(1, n_mp)]
    barrier = pltpu.get_barrier_semaphore()
    for device in others:
        pl.semaphore_signal(barrier, inc=1, device_id=device, device_id_type=MESH)
    pl.semaphore_wait(barrier, len(others))

    def remote(src, dst, send_sem, recv_sem, device):
        return pltpu.make_async_remote_copy(
            src_ref=src, dst_ref=dst, send_sem=send_sem, recv_sem=recv_sem, device_id=device, device_id_type=MESH
        )

    if ring:
        targets = (right, left)
    else:
        targets = [lax.rem(seq + o, n_seq) for o in range(1, w_seq)]
    hops = range(1, n_grp)
    by_seq = 2 if ring and chunks >= 8 and n_grp <= 4 else 0
    by_grp = chunks - by_seq
    seq_first = (chunks - 4, chunks - 2) if by_seq else ()
    plain = by_grp - 2 if by_seq else by_grp

    def nth(a):
        late = 2 * a - plain + 1
        if isinstance(a, int):
            return a if a < plain else late
        return jnp.where(a < plain, a, late)

    def group_of(c):
        if not by_seq:
            return 0
        if isinstance(c, int):
            return int(c in seq_first)
        return ((c == seq_first[0]) | (c == seq_first[1])).astype(jnp.int32)

    def bulk(block, send_sem, recv_sem):
        return remote(block, block, send_sem, recv_sem, {"grp": lax.rem(grp + 1, n_grp)})

    def over_grp(c):
        block = w.at[c, grp, w_pos]
        return [
            remote(block, block, z_send.at[0], z_recv.at[c, o - 1], {"grp": lax.rem(grp + o, n_grp)}) for o in hops
        ]

    def line(c, k):
        ways = []
        b = (c - seq_first[0]) // (seq_first[1] - seq_first[0])
        for i, sign in enumerate((1, -1)):
            source, target = grp - sign * k, grp + sign
            block = w.at[c, jnp.clip(source, 0, n_grp - 1)]
            copy = remote(
                block,
                block,
                l_send.at[b, i, k],
                l_recv.at[b, i, k],
                {"grp": jnp.where(target < 0, 1, jnp.where(target >= n_grp, n_grp - 2, target))},
            )
            sends = (source >= 0) & (source < n_grp) & (target >= 0) & (target < n_grp)
            arrives = (source - sign >= 0) & (source - sign < n_grp)
            ways.append((copy, sends, arrives))
        return ways

    def start_line(c, k):
        if k:
            line_received(c, k - 1)
        for copy, sends, _ in line(c, k):
            pl.when(sends)(copy.start)

    def line_received(c, k):
        for copy, _, arrives in line(c, k):
            pl.when(arrives)(copy.wait_recv)

    def over_seq(c, o):
        block = w.at[c, lax.rem(grp + n_grp - o, n_grp), w_pos]
        return [
            remote(block, block, s_send.at[group_of(c)], s_recv.at[c], {"seq": target}) for target in targets
        ]

    def all_seq(c, grps=slice(None)):
        return [bulk(w.at[c, grps, pl.ds(0, len(targets))], s_send.at[group_of(c)], s_recv.at[c])] if targets else []

    def relay(c, grps=slice(None)):
        if not ring:
            return []
        copies = []
        for i, (source, target) in enumerate(((left, right), (right, left))):
            passed = w.at[c, grps, source, :, pl.ds(i * cols, cols)]
            copies.append(remote(passed, passed, r_send.at[group_of(c)], r_recv.at[c], {"seq": target}))
        return copies

    def all_relay(c, grps=slice(None)):
        return [bulk(w.at[c, grps, 0], r_send.at[group_of(c)], r_recv.at[c])] if ring else []

    def edge_in(c):
        return remote(
            qd.at[:, pl.ds(0, group_len), at(c)],
            edge.at[:, :, at(c)],
            e_send.at[0],
            e_recv.at[c],
            {"seq": preceding},
        )

    def edge_out(c):
        return remote(
            att_out.at[:, at(c)], att_in.at[:, at(c)], a_send.at[0], a_recv.at[0], {"seq": following}
        )

    def start(copies):
        for copy in copies:
            copy.start()

    def received(copies):
        for copy in copies:
            copy.wait_recv()

    def start_seq(c):
        for o, arrival in zip(hops, over_grp(c)):
            arrival.wait_recv()
            start(over_seq(c, o))

    def start_relay(c):
        received(all_seq(c))
        start(relay(c))

    def start_edge(c):
        @pl.when(seq > 0)
        def _():
            edge_in(c).start()

    def arrived(c):
        if isinstance(c, int):
            received(all_relay(c))
        elif not by_seq:
            received(all_relay(c))
        else:
            lined = (c == seq_first[0]) | (c == seq_first[1])

            @pl.when(jnp.logical_not(lined))
            def _():
                received(all_relay(c))

            @pl.when(lined)
            def _():
                line_received(c, n_grp - 2)

        @pl.when(seq < n_seq - 1)
        def _():
            edge_in(c).wait_recv()

    def own_seq(a):
        if a < by_grp:
            start(over_seq(nth(a), 0))

    def own_grp(a):
        start(over_grp(nth(a)))

    own_arrived()
    for c in seq_first:
        start(over_seq(c, 0))
    own_grp(0)
    own_seq(0)
    for a in range(1, min(4, by_grp)):
        own_grp(a)
    own_seq(1)
    for copy in local[:2]:
        copy.wait()

    @pl.when(seq == n_seq - 1)
    def _():
        edge[...] = jnp.zeros_like(edge)

    @pl.when(seq == 0)
    def _():
        att_in[...] = jnp.zeros_like(att_in)

    acc[...] = jnp.zeros_like(acc)
    for c in seq_first:
        received(all_seq(c, 0))
        start(relay(c, grp))
    start_edge(0)
    if chunks > 1:
        start_edge(1)
    own_seq(2)
    start_seq(0)
    own_seq(3)
    for c in seq_first:
        received(all_relay(c, 0))
        start_line(c, 0)
    for a in range(4, by_grp):
        own_grp(a)
    if by_grp > 1:
        start_seq(1)
    start_relay(0)
    if chunks > 2:
        start_edge(2)
    own_seq(4)
    if by_grp > 2:
        start_seq(2)
    for a in range(5, by_grp):
        own_seq(a)
    for copy in local[2:]:
        copy.wait()

    scale = head_dim ** (-0.5)
    folded = scale.hex().startswith("0x1.0000000000000p")
    lane = lax.broadcasted_iota(jnp.int32, (group_len, cols), 1)
    on_first = lane < head_dim
    lane_row = lax.broadcasted_iota(jnp.int32, (1, 2 * group_len), 1)

    def project(c):
        weights = w[c].reshape(enc, 2 * cols)
        states = x[...].reshape(groups * rows, enc)
        kv = dot(states[:, : enc // 2], weights[: enc // 2]) + dot(states[:, enc // 2 :], weights[enc // 2 :])
        k = kv[:, :cols]
        hi = k.astype(jnp.bfloat16)
        key[:, :cols] = hi
        key[:, cols:] = (k - hi.astype(jnp.float32)).astype(jnp.bfloat16)
        value[...] = kv[:, cols:].astype(jnp.bfloat16)

    def attend(c, slots):
        lam = lambdas[c]
        weight = jnp.where(lane_row < group_len, jnp.float32(1.0), -lam)
        unweight = 1.0 / weight
        g = gain[:, at(c)]
        blank = jnp.zeros((2 * group_len, cols), jnp.bfloat16)
        blank_half = jnp.zeros((group_len, cols), jnp.bfloat16)
        here = [slice(u * rows, (u + 1) * rows) for u in slots]
        tokens = [slice((u + 1) * group_len, (u + 2) * group_len) for u in slots]
        active = [jnp.clip(counts[0] - (seq * groups + u + 1), 0, 1).astype(jnp.float32) for u in slots]
        count = range(len(slots))

        def of_tokens(kind, i):
            if slots[i] < groups - 1:
                return qd[kind, tokens[i], at(c)]
            return edge[kind, :, at(c)]

        q2, scores = [], []
        for i in count:
            query = of_tokens(0, i)
            if folded:
                query = (query.astype(jnp.float32) * scale).astype(jnp.bfloat16)
            zero = jnp.zeros_like(query)
            q2.append(jnp.concatenate([jnp.where(on_first, query, zero), jnp.where(on_first, zero, query)], axis=0))
        for i in count:
            scores.append(dot(key[here[i], :], jnp.concatenate([q2[i], q2[i]], axis=1), NT))
            if not folded:
                scores[i] = scores[i] * scale
        e = [jnp.exp(scores[i] - jnp.max(scores[i], axis=0, keepdims=True)) for i in count]
        probs = [e[i] * (weight / jnp.sum(e[i], axis=0, keepdims=True)) for i in count]
        mix = [(probs[i] + pltpu.roll(probs[i], group_len, 1)).astype(jnp.bfloat16) for i in count]
        heads = [dot(mix[i], value[here[i], :], TN)[:group_len] for i in count]
        inverse = [lax.rsqrt(jnp.mean(heads[i] * heads[i], axis=-1, keepdims=True) + EPSILON) for i in count]
        normed = [heads[i] * inverse[i] for i in count]
        dn = [of_tokens(1, i).astype(jnp.float32) * active[i] * g for i in count]
        d_heads = [
            (inverse[i] * (dn[i] - normed[i] * jnp.mean(dn[i] * normed[i], axis=-1, keepdims=True))).astype(
                jnp.bfloat16
            )
            for i in count
        ]
        d_mix = [dot(value[here[i], :], jnp.concatenate([d_heads[i], d_heads[i]], axis=0), NT) for i in count]
        for i in count:
            result = (normed[i] * g * active[i]).astype(jnp.bfloat16)
            if slots[i] < groups - 1:
                att[tokens[i], at(c)] = result
            else:
                att_out[:, at(c)] = result
        total = [jnp.sum(d_mix[i] * probs[i], axis=0, keepdims=True) * unweight for i in count]
        outer = probs if folded else [scale * probs[i] for i in count]
        d_scores = [(outer[i] * (d_mix[i] - total[i])).astype(jnp.bfloat16) for i in count]
        for i in count:
            d_kv[here[i], :cols] = dot(d_scores[i], q2[i]).astype(jnp.bfloat16)
            d_kv[here[i], cols:] = dot(mix[i], jnp.concatenate([d_heads[i], blank_half], axis=0)).astype(jnp.bfloat16)

    def weight_part(c, core):
        part = w[c, pl.ds(core * grp_half, grp_half)]
        return part.reshape(half, 2 * cols)

    def gradients(c):
        for core in range(n_mp):
            acc[core] += dot(d_kv[...], weight_part(c, core), NT)

    def lines(c, i):
        for k in range(1, n_grp - 1):

            @pl.when(c == 2 * k - 1)
            def _(k=k):
                start_line(seq_first[i], k)

    def step(c, first=False, final=False):
        if not final:

            @pl.when(c + 1 < min(plain + 1, by_grp))
            def _():
                start_relay(nth(c + 1))

            @pl.when(c + 3 < plain)
            def _():
                start_seq(nth(c + 3))

            if not first:

                @pl.when((c + 2 >= plain) & (c + 2 < by_grp))
                def _():
                    start_seq(nth(c + 2))

            @pl.when(c + 3 < chunks)
            def _():
                start_edge(c + 3)

        if not first:

            @pl.when(seq < n_seq - 1)
            def _():
                edge_out(c - 1).start()

        if by_seq and not first and not final:
            lines(c, 0)
        arrived(c)
        project(c)
        if not first:
            gradients(c - 1)
        if by_seq and not first and not final:
            lines(c, 1)

            @pl.when(c == plain)
            def _():
                start_relay(nth(plain + 1))

        for u in range(0, groups, TOGETHER):
            attend(c, list(range(u, min(u + TOGETHER, groups))))

    step(0, first=True)

    def loop(c, carry):
        step(c)
        return carry

    lax.fori_loop(1, chunks - 1, loop, 0)
    last = chunks - 1
    step(last, final=True)

    pieces = send.shape[1]
    piece = send.shape[2]

    def exchange(o, i):
        return remote(
            send.at[o - 1, i], got.at[o - 1, i], g_send.at[o - 1, i], g_recv.at[o - 1, i], {"mp": lax.rem(mp + o, n_mp)}
        )

    for o in range(1, n_mp):
        core = lax.rem(mp + o, n_mp)
        for i in range(pieces):
            span = slice(i * piece, (i + 1) * piece)
            part = acc[core, span, :] + dot(d_kv[span, :], weight_part(last, core), NT)
            send[o - 1, i] = part.astype(jnp.bfloat16)
            exchange(o, i).start()

    @pl.when(seq < n_seq - 1)
    def _():
        edge_out(last).start()

    d_out[...] = acc[mp] + dot(d_kv[...], weight_part(last, mp), NT)

    @pl.when(seq > 0)
    def _():
        bulk(att_in, a_send.at[0], a_recv.at[0]).wait_recv()

    att[:group_len, :] = att_in[...]
    for i in range(pieces):
        span = slice(i * piece, (i + 1) * piece)
        total = d_out[span, :]
        for o in range(1, n_mp):
            exchange(o, i).wait()
            total += got[o - 1, i].astype(jnp.float32)
        d_out[span, :] = total

    def sent(copies):
        for copy in copies:
            copy.wait_send()

    for c in seq_first:
        for k in range(n_grp - 1):
            for copy, sends, _ in line(c, k):
                pl.when(sends)(copy.wait_send)
    many = pl.ds(0, by_grp)
    bulk(w.at[many, pl.ds(0, n_grp - 1), w_pos], z_send.at[0], z_recv.at[0, 0]).wait_send()
    if targets:
        bulk(w.at[many, :, pl.ds(0, len(targets))], s_send.at[0], s_recv.at[0]).wait_send()
    if ring:
        bulk(w.at[many, :, 0], r_send.at[0], r_recv.at[0]).wait_send()
    if by_seq:
        bulk(w.at[pl.ds(0, by_seq), 0, pl.ds(0, len(targets))], s_send.at[1], s_recv.at[0]).wait_send()
        bulk(w.at[pl.ds(0, by_seq), 0, 0], r_send.at[1], r_recv.at[0]).wait_send()

    @pl.when(seq > 0)
    def _():
        bulk(edge, e_send.at[0], e_recv.at[0]).wait_send()

    @pl.when(seq < n_seq - 1)
    def _():
        bulk(att_in, a_send.at[0], a_recv.at[0]).wait_send()


def put_out(att, d_neigh, att_hbm, d_hbm, sem):
    copies = [
        pltpu.make_async_copy(d_neigh, d_hbm, sem.at[0]),
        pltpu.make_async_copy(att, att_hbm, sem.at[1]),
    ]
    for copy in copies:
        copy.start()
    for copy in copies:
        copy.wait()


def on_device(mesh_shape, queries, neighbours, w_key, w_value, lambdas, gain, counts, d_out):
    n_grp, n_seq, n_mp = (mesh_shape[name] for name in ("grp", "seq", "mp"))
    groups, rows, enc = neighbours.shape[1:]
    tokens, width = queries.shape[1:]
    w_seq = n_seq
    if w_key.shape[0] % 16:
        w_key = lax.all_gather(w_key, "seq", axis=0, tiled=True)
        w_value = lax.all_gather(w_value, "seq", axis=0, tiled=True)
        w_seq = 1
    w_rows = w_key.shape[0]
    chunks = lambdas.shape[0]
    cols = w_key.shape[1] // chunks
    half = enc // n_mp
    group_len = tokens // groups
    pieces = 2
    bf16, f32 = jnp.bfloat16, jnp.float32
    vmem = pl.BlockSpec(memory_space=pltpu.VMEM)
    hbm = pl.BlockSpec(memory_space=pltpu.HBM)
    dma = pltpu.SemaphoreType.DMA
    att, d_neigh = pl.pallas_call(
        functools.partial(kernel, (n_grp, n_seq, n_mp, w_seq, chunks)),
        out_shape=(
            pltpu.VMEM((tokens, width), bf16),
            pltpu.VMEM((groups * rows, half), f32),
        ),
        in_specs=[hbm] * 8,
        out_specs=(vmem, vmem),
        scratch_shapes=[
            pltpu.SMEM((chunks,), f32),
            pltpu.SMEM((1,), jnp.int32),
            pltpu.VMEM((1, width), f32),
            pltpu.VMEM((groups, rows, enc), bf16),
            pltpu.VMEM((2, tokens, width), bf16),
            pltpu.VMEM((2, group_len, width), bf16),
            pltpu.VMEM((chunks, n_grp, w_seq, w_rows, 2 * cols), bf16),
            pltpu.VMEM((n_mp, groups * rows, half), f32),
            pltpu.VMEM((groups * rows, 2 * cols), bf16),
            pltpu.VMEM((groups * rows, cols), bf16),
            pltpu.VMEM((groups * rows, 2 * cols), bf16),
            pltpu.VMEM((group_len, width), bf16),
            pltpu.VMEM((group_len, width), bf16),
            pltpu.VMEM((n_mp - 1, pieces, groups * rows // pieces, half), bf16),
            pltpu.VMEM((n_mp - 1, pieces, groups * rows // pieces, half), bf16),
            dma((6,)),
            dma((1,)),
            dma((1,)),
            dma((chunks, n_grp - 1)),
            dma((2, 2, n_grp - 1)),
            dma((2, 2, n_grp - 1)),
            dma((2,)),
            dma((chunks,)),
            dma((2,)),
            dma((chunks,)),
            dma((1,)),
            dma((chunks,)),
            dma((1,)),
            dma((1,)),
            dma((n_mp - 1, pieces)),
            dma((n_mp - 1, pieces)),
        ],
        compiler_params=pltpu.CompilerParams(
            collective_id=0, has_side_effects=True, vmem_limit_bytes=64400000
        ),
    )(lambdas, counts, queries[0], neighbours[0], w_key, w_value, gain.reshape(1, -1), d_out[0])
    att, d_neigh = pl.pallas_call(
        put_out,
        out_shape=(
            jax.ShapeDtypeStruct((tokens, width), bf16),
            jax.ShapeDtypeStruct((groups * rows, half), f32),
        ),
        in_specs=[vmem, vmem],
        out_specs=(hbm, hbm),
        scratch_shapes=[dma((2,))],
        compiler_params=pltpu.CompilerParams(vmem_limit_bytes=1024 * 1024),
    )(att, d_neigh)
    return att[None], d_neigh.reshape(1, groups, rows, half)


def solution(mesh):
    in_specs = (
        P("grp", "seq", "mp"),
        P("grp", "seq", None, None),
        P(("grp", "seq"), "mp"),
        P(("grp", "seq"), "mp"),
        P("mp"),
        P("mp"),
        P("grp"),
        P("grp", "seq", "mp"),
    )
    out_specs = (P("grp", "seq", "mp"), P("grp", "seq", None, "mp"))
    return jax.shard_map(
        functools.partial(on_device, dict(mesh.shape)),
        mesh=mesh,
        in_specs=in_specs,
        out_specs=out_specs,
        check_vma=False,
    )
```

```python
import functools

import jax
import jax.numpy as jnp
from jax import lax
from jax.experimental import pallas as pl
from jax.experimental.pallas import tpu as pltpu
from jax.sharding import PartitionSpec as P

EPSILON = 1e-06
TOGETHER = 4
MESH = pl.DeviceIdType.MESH
NT = (((1,), (1,)), ((), ()))
TN = (((0,), (0,)), ((), ()))


def dot(left, right, dims=(((1,), (0,)), ((), ()))):
    return lax.dot_general(left, right, dims, preferred_element_type=jnp.float32)


def kernel(
    sizes,
    lambdas_hbm,
    counts_hbm,
    q_hbm,
    n_hbm,
    wk_hbm,
    wv_hbm,
    gain_hbm,
    do_hbm,
    att,
    d_out,
    lambdas,
    counts,
    gain,
    x,
    qd,
    edge,
    w,
    acc,
    key,
    value,
    d_kv,
    att_out,
    att_in,
    send,
    got,
    local_sem,
    own_sem,
    z_send,
    z_recv,
    l_send,
    l_recv,
    s_send,
    s_recv,
    r_send,
    r_recv,
    e_send,
    e_recv,
    a_send,
    a_recv,
    g_send,
    g_recv,
):
    n_grp, n_seq, n_mp, w_seq, chunks = sizes
    groups, rows, enc = x.shape
    group_len = qd.shape[1] // groups
    cols = w.shape[-1] // 2
    head_dim = cols // 2
    half = enc // n_mp
    grp_half = n_grp // n_mp
    grp, seq, mp = lax.axis_index("grp"), lax.axis_index("seq"), lax.axis_index("mp")
    w_pos = seq if w_seq > 1 else 0
    following = lax.rem(seq + 1, n_seq)
    preceding = lax.rem(seq + n_seq - 1, n_seq)
    ring = w_seq == 4
    if ring:
        right = lax.rem(seq, 2) * 2 + 1 - seq // 2
        left = (1 - lax.rem(seq, 2)) * 2 + seq // 2

    def at(c):
        return pl.ds(pl.multiple_of(c * cols, cols), cols)

    def own(c):
        return [
            pltpu.make_async_copy(
                src.at[:, at(c)], w.at[c, grp, w_pos, :, pl.ds(kind * cols, cols)], own_sem.at[0]
            )
            for kind, src in enumerate((wk_hbm, wv_hbm))
        ]

    def own_arrived():
        block = w.at[:, grp, w_pos]
        pltpu.make_async_copy(block, block, own_sem.at[0]).wait()

    for c in range(chunks):
        for copy in own(c):
            copy.start()
    local = [
        pltpu.make_async_copy(q_hbm, qd.at[0], local_sem.at[0]),
        pltpu.make_async_copy(do_hbm, qd.at[1], local_sem.at[1]),
        pltpu.make_async_copy(n_hbm, x, local_sem.at[2]),
        pltpu.make_async_copy(lambdas_hbm, lambdas, local_sem.at[3]),
        pltpu.make_async_copy(counts_hbm, counts, local_sem.at[4]),
        pltpu.make_async_copy(gain_hbm, gain, local_sem.at[5]),
    ]
    for copy in local:
        copy.start()

    others = [{"grp": lax.rem(grp + o, n_grp)} for o in range(1, n_grp)]
    others += [{"seq": lax.rem(seq + o, n_seq)} for o in (range(1, n_seq) if w_seq > 1 else (1, n_seq - 1))]
    others += [{"mp": lax.rem(mp + o, n_mp)} for o in range(1, n_mp)]
    barrier = pltpu.get_barrier_semaphore()
    for device in others:
        pl.semaphore_signal(barrier, inc=1, device_id=device, device_id_type=MESH)
    pl.semaphore_wait(barrier, len(others))

    def remote(src, dst, send_sem, recv_sem, device):
        return pltpu.make_async_remote_copy(
            src_ref=src, dst_ref=dst, send_sem=send_sem, recv_sem=recv_sem, device_id=device, device_id_type=MESH
        )

    if ring:
        targets = (right, left)
    else:
        targets = [lax.rem(seq + o, n_seq) for o in range(1, w_seq)]
    hops = range(1, n_grp)
    by_seq = 2 if ring and chunks >= 8 and n_grp <= 4 else 0
    by_grp = chunks - by_seq
    seq_first = (chunks - 4, chunks - 2) if by_seq else ()
    plain = by_grp - 2 if by_seq else by_grp

    def nth(a):
        late = 2 * a - plain + 1
        if isinstance(a, int):
            return a if a < plain else late
        return jnp.where(a < plain, a, late)

    def group_of(c):
        if not by_seq:
            return 0
        if isinstance(c, int):
            return int(c in seq_first)
        return ((c == seq_first[0]) | (c == seq_first[1])).astype(jnp.int32)

    def grp_slot(c, o):
        return c * (n_grp - 1) + o - 1 if isinstance(c, int) and c < 2 else c + 2 * (n_grp - 2)

    def bulk(block, send_sem, recv_sem):
        return remote(block, block, send_sem, recv_sem, {"grp": lax.rem(grp + 1, n_grp)})

    def over_grp(c):
        block = w.at[c, grp, w_pos]
        return [
            remote(block, block, z_send.at[0], z_recv.at[grp_slot(c, o)], {"grp": lax.rem(grp + o, n_grp)}) for o in hops
        ]

    def line(c, k):
        ways = []
        b = (c - seq_first[0]) // (seq_first[1] - seq_first[0])
        for i, sign in enumerate((1, -1)):
            source, target = grp - sign * k, grp + sign
            block = w.at[c, jnp.clip(source, 0, n_grp - 1)]
            copy = remote(
                block,
                block,
                l_send.at[b, i, k],
                l_recv.at[b, i, k],
                {"grp": jnp.where(target < 0, 1, jnp.where(target >= n_grp, n_grp - 2, target))},
            )
            sends = (source >= 0) & (source < n_grp) & (target >= 0) & (target < n_grp)
            arrives = (source - sign >= 0) & (source - sign < n_grp)
            ways.append((copy, sends, arrives))
        return ways

    def start_line(c, k):
        if k:
            line_received(c, k - 1)
        for copy, sends, _ in line(c, k):
            pl.when(sends)(copy.start)

    def line_received(c, k):
        for copy, _, arrives in line(c, k):
            pl.when(arrives)(copy.wait_recv)

    def over_seq(c, o):
        block = w.at[c, lax.rem(grp + n_grp - o, n_grp), w_pos]
        return [
            remote(block, block, s_send.at[group_of(c)], s_recv.at[c], {"seq": target}) for target in targets
        ]

    def all_seq(c, grps=slice(None)):
        return [bulk(w.at[c, grps, pl.ds(0, len(targets))], s_send.at[group_of(c)], s_recv.at[c])] if targets else []

    def relay(c, grps=slice(None)):
        if not ring:
            return []
        copies = []
        for i, (source, target) in enumerate(((left, right), (right, left))):
            passed = w.at[c, grps, source, :, pl.ds(i * cols, cols)]
            copies.append(remote(passed, passed, r_send.at[group_of(c)], r_recv.at[c], {"seq": target}))
        return copies

    def all_relay(c, grps=slice(None)):
        return [bulk(w.at[c, grps, 0], r_send.at[group_of(c)], r_recv.at[c])] if ring else []

    def edge_in(c):
        return remote(
            qd.at[:, pl.ds(0, group_len), at(c)],
            edge.at[:, :, at(c)],
            e_send.at[0],
            e_recv.at[c],
            {"seq": preceding},
        )

    def edge_out(c):
        return remote(
            att_out.at[:, at(c)], att_in.at[:, at(c)], a_send.at[0], a_recv.at[0], {"seq": following}
        )

    def start(copies):
        for copy in copies:
            copy.start()

    def received(copies):
        for copy in copies:
            copy.wait_recv()

    def start_seq(c):
        fine = isinstance(c, int) and c < 2
        if not fine:
            bulk(w.at[c, pl.ds(0, n_grp - 1), w_pos], z_send.at[0], z_recv.at[grp_slot(c, 1)]).wait_recv()
        for o, arrival in zip(hops, over_grp(c)):
            if fine:
                arrival.wait_recv()
            start(over_seq(c, o))

    def start_relay(c):
        received(all_seq(c))
        start(relay(c))

    def start_edge(c):
        @pl.when(seq > 0)
        def _():
            edge_in(c).start()

    def arrived(c):
        if isinstance(c, int):
            received(all_relay(c))
        elif not by_seq:
            received(all_relay(c))
        else:
            lined = (c == seq_first[0]) | (c == seq_first[1])

            @pl.when(jnp.logical_not(lined))
            def _():
                received(all_relay(c))

            @pl.when(lined)
            def _():
                line_received(c, n_grp - 2)

        @pl.when(seq < n_seq - 1)
        def _():
            edge_in(c).wait_recv()

    def own_seq(a):
        if a < by_grp:
            start(over_seq(nth(a), 0))

    def own_grp(a):
        start(over_grp(nth(a)))

    own_arrived()
    for c in seq_first:
        start(over_seq(c, 0))
    own_grp(0)
    own_seq(0)
    for a in range(1, min(4, by_grp)):
        own_grp(a)
    own_seq(1)
    for copy in local[:2]:
        copy.wait()

    @pl.when(seq == n_seq - 1)
    def _():
        edge[...] = jnp.zeros_like(edge)

    @pl.when(seq == 0)
    def _():
        att_in[...] = jnp.zeros_like(att_in)

    acc[...] = jnp.zeros_like(acc)
    for c in seq_first:
        received(all_seq(c, 0))
        start(relay(c, grp))
    start_edge(0)
    if chunks > 1:
        start_edge(1)
    own_seq(2)
    start_seq(0)
    own_seq(3)
    for c in seq_first:
        received(all_relay(c, 0))
        start_line(c, 0)
    for a in range(4, by_grp):
        own_grp(a)
    if by_grp > 1:
        start_seq(1)
    start_relay(0)
    if chunks > 2:
        start_edge(2)
    own_seq(4)
    if by_grp > 2:
        start_seq(2)
    for a in range(5, by_grp):
        own_seq(a)
    for copy in local[2:]:
        copy.wait()

    scale = head_dim ** (-0.5)
    folded = scale.hex().startswith("0x1.0000000000000p")
    lane = lax.broadcasted_iota(jnp.int32, (group_len, cols), 1)
    on_first = lane < head_dim
    lane_row = lax.broadcasted_iota(jnp.int32, (1, 2 * group_len), 1)

    def project(c):
        weights = w[c].reshape(enc, 2 * cols)
        states = x[...].reshape(groups * rows, enc)
        kv = dot(states[:, : enc // 2], weights[: enc // 2]) + dot(states[:, enc // 2 :], weights[enc // 2 :])
        k = kv[:, :cols]
        hi = k.astype(jnp.bfloat16)
        key[:, :cols] = hi
        key[:, cols:] = (k - hi.astype(jnp.float32)).astype(jnp.bfloat16)
        value[...] = kv[:, cols:].astype(jnp.bfloat16)

    def attend(c, slots):
        lam = lambdas[c]
        weight = jnp.where(lane_row < group_len, jnp.float32(1.0), -lam)
        unweight = 1.0 / weight
        g = gain[:, at(c)]
        blank = jnp.zeros((2 * group_len, cols), jnp.bfloat16)
        blank_half = jnp.zeros((group_len, cols), jnp.bfloat16)
        here = [slice(u * rows, (u + 1) * rows) for u in slots]
        tokens = [slice((u + 1) * group_len, (u + 2) * group_len) for u in slots]
        active = [jnp.clip(counts[0] - (seq * groups + u + 1), 0, 1).astype(jnp.float32) for u in slots]
        count = range(len(slots))

        def of_tokens(kind, i):
            if slots[i] < groups - 1:
                return qd[kind, tokens[i], at(c)]
            return edge[kind, :, at(c)]

        q2, scores = [], []
        for i in count:
            query = of_tokens(0, i)
            if folded:
                query = (query.astype(jnp.float32) * scale).astype(jnp.bfloat16)
            zero = jnp.zeros_like(query)
            q2.append(jnp.concatenate([jnp.where(on_first, query, zero), jnp.where(on_first, zero, query)], axis=0))
        for i in count:
            scores.append(dot(key[here[i], :], jnp.concatenate([q2[i], q2[i]], axis=1), NT))
            if not folded:
                scores[i] = scores[i] * scale
        e = [jnp.exp(scores[i] - jnp.max(scores[i], axis=0, keepdims=True)) for i in count]
        probs = [e[i] * (weight / jnp.sum(e[i], axis=0, keepdims=True)) for i in count]
        mix = [(probs[i] + pltpu.roll(probs[i], group_len, 1)).astype(jnp.bfloat16) for i in count]
        heads = [dot(mix[i], value[here[i], :], TN)[:group_len] for i in count]
        inverse = [lax.rsqrt(jnp.mean(heads[i] * heads[i], axis=-1, keepdims=True) + EPSILON) for i in count]
        normed = [heads[i] * inverse[i] for i in count]
        dn = [of_tokens(1, i).astype(jnp.float32) * active[i] * g for i in count]
        d_heads = [
            (inverse[i] * (dn[i] - normed[i] * jnp.mean(dn[i] * normed[i], axis=-1, keepdims=True))).astype(
                jnp.bfloat16
            )
            for i in count
        ]
        d_mix = [dot(value[here[i], :], jnp.concatenate([d_heads[i], d_heads[i]], axis=0), NT) for i in count]
        for i in count:
            result = (normed[i] * g * active[i]).astype(jnp.bfloat16)
            if slots[i] < groups - 1:
                att[tokens[i], at(c)] = result
            else:
                att_out[:, at(c)] = result
        total = [jnp.sum(d_mix[i] * probs[i], axis=0, keepdims=True) * unweight for i in count]
        outer = probs if folded else [scale * probs[i] for i in count]
        d_scores = [(outer[i] * (d_mix[i] - total[i])).astype(jnp.bfloat16) for i in count]
        for i in count:
            d_kv[here[i], :cols] = dot(d_scores[i], q2[i]).astype(jnp.bfloat16)
            d_kv[here[i], cols:] = dot(mix[i], jnp.concatenate([d_heads[i], blank_half], axis=0)).astype(jnp.bfloat16)

    def weight_part(c, core):
        part = w[c, pl.ds(core * grp_half, grp_half)]
        return part.reshape(half, 2 * cols)

    def gradients(c):
        for core in range(n_mp):
            acc[core] += dot(d_kv[...], weight_part(c, core), NT)

    def lines(c, i):
        for k in range(1, n_grp - 1):

            @pl.when(c == 2 * k - 1)
            def _(k=k):
                start_line(seq_first[i], k)

    def step(c, first=False, final=False):
        if not final:

            @pl.when(c + 1 < min(plain + 1, by_grp))
            def _():
                start_relay(nth(c + 1))

            @pl.when(c + 3 < plain)
            def _():
                start_seq(nth(c + 3))

            if not first:

                @pl.when((c + 2 >= plain) & (c + 2 < by_grp))
                def _():
                    start_seq(nth(c + 2))

            @pl.when(c + 3 < chunks)
            def _():
                start_edge(c + 3)

        if not first:

            @pl.when(seq < n_seq - 1)
            def _():
                edge_out(c - 1).start()

        if by_seq and not first and not final:
            lines(c, 0)
        arrived(c)
        project(c)
        if not first:
            gradients(c - 1)
        if by_seq and not first and not final:
            lines(c, 1)

            @pl.when(c == plain)
            def _():
                start_relay(nth(plain + 1))

        for u in range(0, groups, TOGETHER):
            attend(c, list(range(u, min(u + TOGETHER, groups))))

    step(0, first=True)

    def loop(c, carry):
        step(c)
        return carry

    lax.fori_loop(1, chunks - 1, loop, 0)
    last = chunks - 1
    step(last, final=True)

    pieces = send.shape[1]
    piece = send.shape[2]

    def exchange(o, i):
        return remote(
            send.at[o - 1, i], got.at[o - 1, i], g_send.at[o - 1, i], g_recv.at[o - 1, i], {"mp": lax.rem(mp + o, n_mp)}
        )

    for o in range(1, n_mp):
        core = lax.rem(mp + o, n_mp)
        for i in range(pieces):
            span = slice(i * piece, (i + 1) * piece)
            part = acc[core, span, :] + dot(d_kv[span, :], weight_part(last, core), NT)
            send[o - 1, i] = part.astype(jnp.bfloat16)
            exchange(o, i).start()

    @pl.when(seq < n_seq - 1)
    def _():
        edge_out(last).start()

    d_out[...] = acc[mp] + dot(d_kv[...], weight_part(last, mp), NT)

    @pl.when(seq > 0)
    def _():
        bulk(att_in, a_send.at[0], a_recv.at[0]).wait_recv()

    att[:group_len, :] = att_in[...]
    for i in range(pieces):
        span = slice(i * piece, (i + 1) * piece)
        total = d_out[span, :]
        for o in range(1, n_mp):
            exchange(o, i).wait()
            total += got[o - 1, i].astype(jnp.float32)
        d_out[span, :] = total

    def sent(copies):
        for copy in copies:
            copy.wait_send()

    for c in seq_first:
        for k in range(n_grp - 1):
            for copy, sends, _ in line(c, k):
                pl.when(sends)(copy.wait_send)
    many = pl.ds(0, by_grp)
    bulk(w.at[many, pl.ds(0, n_grp - 1), w_pos], z_send.at[0], z_recv.at[0]).wait_send()
    if targets:
        bulk(w.at[many, :, pl.ds(0, len(targets))], s_send.at[0], s_recv.at[0]).wait_send()
    if ring:
        bulk(w.at[many, :, 0], r_send.at[0], r_recv.at[0]).wait_send()
    if by_seq:
        bulk(w.at[pl.ds(0, by_seq), 0, pl.ds(0, len(targets))], s_send.at[1], s_recv.at[0]).wait_send()
        bulk(w.at[pl.ds(0, by_seq), 0, 0], r_send.at[1], r_recv.at[0]).wait_send()

    @pl.when(seq > 0)
    def _():
        bulk(edge, e_send.at[0], e_recv.at[0]).wait_send()

    @pl.when(seq < n_seq - 1)
    def _():
        bulk(att_in, a_send.at[0], a_recv.at[0]).wait_send()


def put_out(att, d_neigh, att_hbm, d_hbm, sem):
    copies = [
        pltpu.make_async_copy(d_neigh, d_hbm, sem.at[0]),
        pltpu.make_async_copy(att, att_hbm, sem.at[1]),
    ]
    for copy in copies:
        copy.start()
    for copy in copies:
        copy.wait()


def on_device(mesh_shape, queries, neighbours, w_key, w_value, lambdas, gain, counts, d_out):
    n_grp, n_seq, n_mp = (mesh_shape[name] for name in ("grp", "seq", "mp"))
    groups, rows, enc = neighbours.shape[1:]
    tokens, width = queries.shape[1:]
    w_seq = n_seq
    if w_key.shape[0] % 16:
        w_key = lax.all_gather(w_key, "seq", axis=0, tiled=True)
        w_value = lax.all_gather(w_value, "seq", axis=0, tiled=True)
        w_seq = 1
    w_rows = w_key.shape[0]
    chunks = lambdas.shape[0]
    cols = w_key.shape[1] // chunks
    half = enc // n_mp
    group_len = tokens // groups
    pieces = 2
    bf16, f32 = jnp.bfloat16, jnp.float32
    vmem = pl.BlockSpec(memory_space=pltpu.VMEM)
    hbm = pl.BlockSpec(memory_space=pltpu.HBM)
    dma = pltpu.SemaphoreType.DMA
    att, d_neigh = pl.pallas_call(
        functools.partial(kernel, (n_grp, n_seq, n_mp, w_seq, chunks)),
        out_shape=(
            pltpu.VMEM((tokens, width), bf16),
            pltpu.VMEM((groups * rows, half), f32),
        ),
        in_specs=[hbm] * 8,
        out_specs=(vmem, vmem),
        scratch_shapes=[
            pltpu.SMEM((chunks,), f32),
            pltpu.SMEM((1,), jnp.int32),
            pltpu.VMEM((1, width), f32),
            pltpu.VMEM((groups, rows, enc), bf16),
            pltpu.VMEM((2, tokens, width), bf16),
            pltpu.VMEM((2, group_len, width), bf16),
            pltpu.VMEM((chunks, n_grp, w_seq, w_rows, 2 * cols), bf16),
            pltpu.VMEM((n_mp, groups * rows, half), f32),
            pltpu.VMEM((groups * rows, 2 * cols), bf16),
            pltpu.VMEM((groups * rows, cols), bf16),
            pltpu.VMEM((groups * rows, 2 * cols), bf16),
            pltpu.VMEM((group_len, width), bf16),
            pltpu.VMEM((group_len, width), bf16),
            pltpu.VMEM((n_mp - 1, pieces, groups * rows // pieces, half), bf16),
            pltpu.VMEM((n_mp - 1, pieces, groups * rows // pieces, half), bf16),
            dma((6,)),
            dma((1,)),
            dma((1,)),
            dma((chunks + 2 * (n_grp - 2),)),
            dma((2, 2, n_grp - 1)),
            dma((2, 2, n_grp - 1)),
            dma((2,)),
            dma((chunks,)),
            dma((2,)),
            dma((chunks,)),
            dma((1,)),
            dma((chunks,)),
            dma((1,)),
            dma((1,)),
            dma((n_mp - 1, pieces)),
            dma((n_mp - 1, pieces)),
        ],
        compiler_params=pltpu.CompilerParams(
            collective_id=0, has_side_effects=True, vmem_limit_bytes=64400000
        ),
    )(lambdas, counts, queries[0], neighbours[0], w_key, w_value, gain.reshape(1, -1), d_out[0])
    att, d_neigh = pl.pallas_call(
        put_out,
        out_shape=(
            jax.ShapeDtypeStruct((tokens, width), bf16),
            jax.ShapeDtypeStruct((groups * rows, half), f32),
        ),
        in_specs=[vmem, vmem],
        out_specs=(hbm, hbm),
        scratch_shapes=[dma((2,))],
        compiler_params=pltpu.CompilerParams(vmem_limit_bytes=1024 * 1024),
    )(att, d_neigh)
    return att[None], d_neigh.reshape(1, groups, rows, half)


def solution(mesh):
    in_specs = (
        P("grp", "seq", "mp"),
        P("grp", "seq", None, None),
        P(("grp", "seq"), "mp"),
        P(("grp", "seq"), "mp"),
        P("mp"),
        P("mp"),
        P("grp"),
        P("grp", "seq", "mp"),
    )
    out_specs = (P("grp", "seq", "mp"), P("grp", "seq", None, "mp"))
    return jax.shard_map(
        functools.partial(on_device, dict(mesh.shape)),
        mesh=mesh,
        in_specs=in_specs,
        out_specs=out_specs,
        check_vma=False,
    )
```
